128 devices in a mesh: emb: 8 (over x, core), seq: 16 (over z, y).
Axes of the slice: x: 4, y: 4, z: 4, core: 2. Of those that a mesh axis runs over, the one named last changes fastest.
Arguments:
- token_rows: int32 [8, 8192], P('emb', 'seq'), may hold values from 0 to 4607, as said below
- segment_ids: int32 [8, 8192], P('emb', 'seq'), may hold values from 0 to 3, never falling along the last dimension, each value on 1 to 4096 neighbouring positions
- requests: int32 [128, 128, 4], P(('emb', 'seq')), may hold values from 0 to 8191, as said below
- hot_table: bfloat16 [4096, 512], replicated, may hold values from -6 to 6
- cold_table: bfloat16 [1048576, 512], P(('emb', 'seq')), may hold values from -6 to 6
- input_weight: bfloat16 [512, 2048], replicated, may hold values from -0.75 to 0.75
- output_weight: bfloat16 [512, 512], replicated, may hold values from -0.25 to 0.25
- up_weight: bfloat16 [512, 2048], replicated, may hold values from -0.25 to 0.25
- down_weight: bfloat16 [2048, 512], replicated, may hold values from -0.125 to 0.125
Outputs:
- layer_output: bfloat16 [8, 8192, 512], P('emb', 'seq')
The draws below stay inside these ranges and needn't reach their ends.
Inputs may be any that keep to these rules, and one draw needn't show every extreme that they name: `token_rows`: A value below 4096 names that row of hot_table. A value 4096 + o * 4 + k names slot k of the holding device's requests to owner o, and that slot is always a live one. Exactly 256 positions of each device name request slots. For each requesting device and owner the live requests fill slots 0 to c - 1, with c from 1 to 4; dead slots hold 0. Some owners, the same ones for all requesters, get all 4 slots live from every device, and every draw has at least one such owner. `segment_ids`: segment numbers never fall along a sequence.
All inputs are finite; a program needn't handle non-finite values.
Results may differ from the reference program's by a relative error of at most 0.0087.
Values may be sent and summed in bfloat16 or wider, within the bound.
A program may use at most 128 MiB of HBM per device.

```python
import math
import jax
import jax.numpy as jnp
import numpy as np
from jax import lax

D = 512
H = 16
FF = 2048
HOT = 4096
COLD_DEV = 8192
CAP = 4
SEQ_DEV = 512
L = 8192
N_EMB = 8
N_SEQ = 16
DEVICES = 128


def plan_tokens(key):
    folded = jax.random.fold_in(key, 4099)
    subkeys = jax.random.split(folded, 6)
    owners = jnp.arange(DEVICES, dtype=jnp.int32)
    heavy_owner = jax.random.randint(subkeys[0], (DEVICES,), 0, 4) == 0
    forced = jax.random.randint(subkeys[1], (), 0, DEVICES)
    heavy_owner = heavy_owner | (owners == forced)
    light_count = jax.random.randint(subkeys[2], (DEVICES, DEVICES), 1, CAP // 2 + 1)
    counts = jnp.where(heavy_owner[None, :], CAP, light_count)
    slot_index = jnp.arange(DEVICES * CAP, dtype=jnp.int32)
    live_slot = (slot_index % CAP)[None, :] < jnp.repeat(counts, CAP, axis=1)
    wanted = jax.random.randint(subkeys[3], (DEVICES, DEVICES * CAP), 0, COLD_DEV)
    requests = jnp.where(live_slot, wanted, 0).reshape(DEVICES, DEVICES, CAP).astype(jnp.int32)
    live_order = jnp.argsort(1 - live_slot.astype(jnp.int32), axis=1, stable=True).astype(jnp.int32)
    live_total = jnp.sum(live_slot.astype(jnp.int32), axis=1)
    shuffle_keys = jax.random.randint(subkeys[4], (DEVICES, SEQ_DEV), 0, 1 << 20) * SEQ_DEV + jnp.arange(SEQ_DEV, dtype=jnp.int32)[None, :]
    token_rank = jnp.argsort(jnp.argsort(shuffle_keys, axis=1, stable=True), axis=1, stable=True).astype(jnp.int32)
    is_cold = token_rank < SEQ_DEV // 2
    picked = jnp.take_along_axis(live_order, token_rank % live_total[:, None], axis=1)
    hot_choice = jax.random.randint(subkeys[5], (DEVICES, SEQ_DEV), 0, HOT)
    item_ids = jnp.where(is_cold, HOT + picked, hot_choice).astype(jnp.int32)
    return (requests, item_ids.reshape(N_EMB, SEQ_DEV * N_SEQ))


def draw_token_rows(key, part):
    return plan_tokens(key)[1]


def draw_requests(key, part):
    return plan_tokens(key)[0]


def levels(key, extent, cuts, low, largest):
    loudness, own = 1.0, jax.random.fold_in(key, 6)
    for dim, blocks in cuts:
        heights = jnp.exp(jax.random.uniform(jax.random.fold_in(own, dim), (blocks,), jnp.float32, low / len(cuts), largest / len(cuts)))
        loudness = loudness * jnp.repeat(heights, extent[dim] // blocks).reshape([-1 if axis == dim else 1 for axis in range(len(extent))])
    return loudness


def length_profile(count, total, reach, slope):
    portions = [(1 << 20) // math.isqrt(rank ** slope) + 1 for rank in range(2, count + 1)]
    surplus, holding = total - reach - (count - 1), [1] * (count - 1)
    while surplus > 0:
        free = [i for i in range(count - 1) if holding[i] < reach]
        whole, budget = sum([portions[i] for i in free]), surplus
        for i in free:
            more = min(reach - holding[i], max(1, budget * portions[i] // whole), surplus)
            holding[i] = holding[i] + more
            surplus = surplus - more
    return np.array([reach] + holding)


def ragged(rng, amount, total, most, skew):
    if amount == 2:
        one = jax.random.randint(rng, (), max(1, total - most), min(most, total - 1) + 1)
        return jnp.stack([one, total - one])
    lengths = jnp.asarray(length_profile(amount, total, most, skew), jnp.int32)
    pairs = (amount - 1) // 2
    giver, receiver = lengths[1:1 + 2 * pairs:2], lengths[2:2 + 2 * pairs:2]
    room = jnp.minimum(giver - 1, most - receiver)
    moved = jax.random.randint(jax.random.fold_in(rng, 1), (pairs,), 0, 1 << 20) % (room + 1)
    lengths = lengths.at[1:1 + 2 * pairs:2].set(giver - moved).at[2:2 + 2 * pairs:2].set(receiver + moved)
    return lengths[jax.random.permutation(jax.random.fold_in(rng, 2), amount)]


def noise(rng, shape, width, reach, pieces=(), kind=jnp.bfloat16):
    values = jax.random.normal(rng, shape, jnp.float32) * width
    if len(pieces) > 0:
        values = levels(rng, shape, pieces, -0.22, 0.18) * values
    return jnp.clip(values, min=-reach, max=reach).astype(kind)


def setup_inputs(seed: int = 0) -> dict:
    streams_of = jax.random.split(jax.random.key(seed), 10)
    return {
        "token_rows": draw_token_rows(jax.random.fold_in(streams_of[9], 71), 0),
        "segment_ids": jax.vmap(lambda own: jnp.searchsorted(jnp.cumsum(ragged(own, 4, L, L // 2, 0)), jnp.arange(L), side="right"))(jax.random.split(streams_of[1], N_EMB)).reshape((N_EMB, L)).astype(jnp.int32),
        "requests": draw_requests(jax.random.fold_in(streams_of[9], 71), 0),
        "hot_table": noise(streams_of[3], (HOT, D), 1.0, 6.0),
        "cold_table": noise(streams_of[4], (DEVICES * COLD_DEV, D), 1.0, 6.0, ((0, 128),)),
        "input_weight": noise(streams_of[5], (D, 4 * D), (D // 9) ** -0.5, 0.75),
        "output_weight": noise(streams_of[6], (D, D), D ** -0.5, 0.25),
        "up_weight": noise(streams_of[7], (D, FF), D ** -0.5, 0.25),
        "down_weight": noise(streams_of[8], (FF, D), FF ** -0.5, 0.125),
    }


epsilon = 1e-06

def normalize(values):
    widened = values.astype(jnp.float32)
    return widened * lax.rsqrt(lax.optimization_barrier(jnp.mean(widened * widened, axis=-1, keepdims=True)) + epsilon)

def reference(token_rows, segment_ids, requests, hot_table, cold_table, input_weight, output_weight, up_weight, down_weight):
    length = SEQ_DEV * N_SEQ
    block_rows = math.gcd(length, 1024)
    blocks = length // block_rows
    head_width = D // H
    score_scale = 1.0 / math.sqrt(head_width)
    flat_requests = requests.reshape(DEVICES, DEVICES * CAP)
    places = jnp.arange(length, dtype=jnp.int32)
    offsets = jnp.arange(block_rows, dtype=jnp.int32)

    def one_sequence(inputs):
        item_ids, segments, member = inputs
        device = member * N_SEQ + places // SEQ_DEV
        is_hot = item_ids < HOT
        slot_index = jnp.where(is_hot, 0, item_ids - HOT)
        local_row = flat_requests[device, slot_index]
        cold_rows = cold_table[slot_index // CAP * COLD_DEV + local_row]
        hot_rows = hot_table[jnp.where(is_hot, item_ids, 0)]
        embedded = jnp.where(is_hot[:, None], hot_rows, cold_rows)
        normed_input = normalize(embedded).astype(jnp.bfloat16)
        projected = jnp.dot(normed_input, input_weight, preferred_element_type=jnp.float32).astype(jnp.bfloat16)
        projected = lax.optimization_barrier(projected).reshape(length, H, 4, head_width)
        gate_units = jax.nn.silu(projected[:, :, 0].astype(jnp.float32)).reshape(length, D)
        heads_first = jnp.moveaxis(projected[:, :, 1:], 1, 0)

        def one_head(head_rows):
            value_rows = head_rows[:, 0].astype(jnp.float32)
            query_rows = head_rows[:, 1].astype(jnp.float32)
            key_rows = head_rows[:, 2].astype(jnp.float32)

            def one_block(block_inputs):
                query_block, query_segments, position = block_inputs
                query_places = position * block_rows + offsets
                scores = jnp.dot(query_block, key_rows.T, preferred_element_type=jnp.float32) * score_scale
                allowed = (places[None, :] <= query_places[:, None]) & (query_segments[:, None] == segments[None, :])
                weights = jnp.where(allowed, jax.nn.silu(scores), 0.0).astype(jnp.bfloat16)
                weights = lax.optimization_barrier(weights).astype(jnp.float32)
                return jnp.dot(weights, value_rows, preferred_element_type=jnp.float32).astype(jnp.bfloat16)
            outputs = lax.map(one_block, (query_rows.reshape(blocks, block_rows, head_width), segments.reshape(blocks, block_rows), jnp.arange(blocks, dtype=jnp.int32)))
            return outputs.reshape(length, head_width)
        attended = lax.map(one_head, heads_first)
        attended = jnp.moveaxis(attended, 0, 1).reshape(length, D).astype(jnp.float32)
        mean_square = lax.optimization_barrier(jnp.mean(attended * attended, axis=-1, keepdims=True))
        normed_heads = (attended * lax.rsqrt(mean_square + epsilon) * gate_units).astype(jnp.bfloat16)
        hidden = embedded.astype(jnp.float32) + jnp.dot(normed_heads, output_weight, preferred_element_type=jnp.float32)
        normed_hidden = normalize(hidden).astype(jnp.bfloat16)
        activated = jax.nn.silu(jnp.dot(normed_hidden, up_weight, preferred_element_type=jnp.float32)).astype(jnp.bfloat16)
        return (hidden + jnp.dot(activated, down_weight, preferred_element_type=jnp.float32)).astype(jnp.bfloat16)
    return lax.map(one_sequence, (token_rows, segment_ids, jnp.arange(N_EMB, dtype=jnp.int32)))
```

```python
import functools
import math

import jax
import jax.numpy as jnp
from jax import lax
from jax.experimental import pallas as pl
from jax.experimental.pallas import tpu as pltpu
from jax.sharding import PartitionSpec as P

H = 16
epsilon = 1e-06

BIG = float(2 ** 30)

def attn_kernel(TQ, TK, U, BF, starts_ref, qkv_ref, out_ref, q_scr, k_scr, v_scr, m_scr, a_scr, acc_scr):
    nb, _, W = qkv_ref.shape
    L = nb * W
    NQ = L // TQ
    s1, s2, s3 = starts_ref[0], starts_ref[1], starts_ref[2]
    C = 0.5 / (32.0 ** 0.5)
    bf = jnp.bfloat16

    def prep(b, _):
        base = b * W
        lane = lax.broadcasted_iota(jnp.int32, (16, W), 1) + base
        row = lax.broadcasted_iota(jnp.int32, (16, W), 0)
        seg = (lane >= s1).astype(jnp.int32) + (lane >= s2).astype(jnp.int32) + (lane >= s3).astype(jnp.int32)
        hot = (seg == row).astype(jnp.float32)
        q = qkv_ref[b, 32:64, :].astype(jnp.float32) * C
        qx = jnp.concatenate([q.astype(bf), hot.astype(bf)], axis=0)
        for c in range(W // 256):
            q_scr[b * (W // 256) + c] = qx[:, c * 256:(c + 1) * 256]
        bias = jnp.where(row < 4, (1.0 - hot) * (-BIG), 0.0)
        kx = jnp.concatenate([qkv_ref[b, 64:96, :].astype(jnp.float32), bias], axis=0)
        k_scr[pl.ds(base, W), :] = kx.T.astype(bf)
        v = qkv_ref[b, 0:32, :]
        for c in range(W // 256):
            v_scr[b * (W // 256) + c] = v[:, c * 256:(c + 1) * 256]
        return 0
    lax.fori_loop(0, nb, prep, 0)

    R = TQ // TK
    for r in range(R):
        t = lax.broadcasted_iota(jnp.int32, (TK, TQ), 0) + r * TK
        qq = lax.broadcasted_iota(jnp.int32, (TK, TQ), 1)
        m_scr[r] = (t <= qq).astype(jnp.float32).astype(bf)
    m_scr[R] = jnp.ones((TK, TQ), bf)
    m_scr[R + 1] = jnp.zeros((TK, TQ), bf)

    def lo_of(i):
        p0 = i * TQ
        st = jnp.where(p0 >= s3, s3, jnp.where(p0 >= s2, s2, jnp.where(p0 >= s1, s1, 0)))
        return st // TK

    def count(i, n):
        return n + (i * R + R - lo_of(i))
    total = lax.fori_loop(0, NQ, count, 0)
    steps = (total + U - 1) // U

    def nxt(i, j):
        last = j <= lo_of(i)
        i2 = jnp.where(last, i + 1, i)
        j2 = jnp.where(last, (i + 1) * R + R - 1, j - 1)
        return i2, j2

    qh = TQ // 256
    kh = TK // 256

    def make(slot, i, j, valid):
        d = j - i * R
        ms = jnp.where(valid, jnp.where(d >= 0, d, R), R + 1)
        k = k_scr[pl.ds(j * TK, TK), :]
        for c in range(qh):
            q = q_scr[i * qh + c]
            s = jnp.dot(k, q, preferred_element_type=jnp.float32)
            if BF:
                h = s.astype(bf)
                a = h + h * jnp.tanh(h)
            else:
                a = (s + s * jnp.tanh(s)).astype(bf)
            a = a * m_scr[ms, :, c * 256:(c + 1) * 256]
            a_scr[slot, :, c * 256:(c + 1) * 256] = a

    def consume(slot, i, j, valid):
        first = j == i * R + R - 1
        for c in range(qh):
            o = jnp.where(first, 0.0, acc_scr[:, c * 256:(c + 1) * 256])
            for t in range(kh):
                o = o + jnp.dot(v_scr[j * kh + t], a_scr[slot, t * 256:(t + 1) * 256, c * 256:(c + 1) * 256],
                                preferred_element_type=jnp.float32)
            acc_scr[:, c * 256:(c + 1) * 256] = o
            if TQ <= W:
                bi = i // (W // TQ)
                if W == TQ:
                    out_ref[bi, :, c * 256:(c + 1) * 256] = o.astype(bf)
                else:
                    off = pl.multiple_of((i % (W // TQ)) * TQ, 256)
                    out_ref[bi, :, pl.ds(off, 256)] = o.astype(bf)
            else:
                out_ref[i * (TQ // W) + (c * 256) // W, :, (c * 256) % W:(c * 256) % W + 256] = o.astype(bf)

    def seq(n0, i, j):
        out = []
        for u in range(U):
            valid = n0 + u < total
            ic = jnp.where(valid, i, 0)
            jc = jnp.where(valid, j, 0)
            out.append((i, j, valid))
            i, j = nxt(i, j)
        return out, i, j

    def clamp(i, j, valid):
        return jnp.minimum(i, NQ - 1), jnp.where(valid, j, 0)

    i0 = jnp.int32(0); j0 = jnp.int32(R - 1)
    lst, i1, j1 = seq(0, i0, j0)
    for u, (i, j, v) in enumerate(lst):
        ci, cj = clamp(i, j, v)
        make(u, ci, cj, v)

    def body(n, carry):
        i, j, ni, nj = carry
        lst, _, _ = seq(n * U, i, j)
        lst2, n2i, n2j = seq((n + 1) * U, ni, nj)
        for u in range(U):
            ci, cj = clamp(*lst[u])
            consume(u, ci, cj, lst[u][2])
        for u in range(U):
            ci, cj = clamp(*lst2[u])
            make(u, ci, cj, lst2[u][2])
        return (ni, nj, n2i, n2j)
    lax.fori_loop(0, steps, body, (i0, j0, i1, j1))


def attention(starts, qkv, TQ=512, TK=512, U=1, BF=True):
    nb, _, W = qkv.shape
    L = nb * W
    bf = jnp.bfloat16
    R = TQ // TK
    return pl.pallas_call(
        functools.partial(attn_kernel, TQ, TK, U, BF),
        out_shape=jax.ShapeDtypeStruct((nb, 32, W), bf),
        in_specs=[pl.BlockSpec(memory_space=pltpu.SMEM), pl.BlockSpec(memory_space=pltpu.VMEM)],
        out_specs=pl.BlockSpec(memory_space=pltpu.VMEM),
        scratch_shapes=[
            pltpu.VMEM((L // 256, 48, 256), bf),
            pltpu.VMEM((L, 48), bf),
            pltpu.VMEM((L // 256, 32, 256), bf),
            pltpu.VMEM((R + 2, TK, TQ), bf),
            pltpu.VMEM((U, TK, TQ), bf),
            pltpu.VMEM((32, TQ), jnp.float32),
        ],
        compiler_params=pltpu.CompilerParams(vmem_limit_bytes=60 << 20),
        name="attn",
    )(starts, qkv)


MESH = pl.DeviceIdType.MESH


def greet(axis_size):
    me = lax.axis_index("seq")
    barrier = pltpu.get_barrier_semaphore()

    def signal(step, carry):
        peer = lax.rem(me + step, axis_size)
        pl.semaphore_signal(barrier, inc=1, device_id={"seq": peer}, device_id_type=MESH)
        return carry

    lax.fori_loop(1, axis_size, signal, 0)
    pl.semaphore_wait(barrier, axis_size - 1)


def project_kernel(n, emb_ref, w_hbm, count_ref, gate_ref, recv_ref, counts_ref, w_ref, x_ref, send, sends, recvs, csends, crecvs, wsem, lsem):
    me = lax.axis_index("seq")
    load = pltpu.make_async_copy(w_hbm, w_ref, wsem)
    load.start()
    greet(n)

    def count_copy(step, src):
        peer = lax.rem(me + step, n)
        return pltpu.make_async_remote_copy(
            src_ref=count_ref, dst_ref=counts_ref.at[src], send_sem=csends.at[peer], recv_sem=crecvs.at[src],
            device_id={"seq": peer}, device_id_type=MESH,
        )

    def start_count(step, carry):
        count_copy(step, me).start()
        return carry

    lax.fori_loop(1, n, start_count, 0)
    counts_ref[me] = count_ref[...]
    x = emb_ref[...].astype(jnp.float32)
    x_ref[...] = (x * lax.rsqrt(jnp.mean(x * x, axis=-1, keepdims=True) + epsilon)).astype(jnp.bfloat16)
    load.wait()

    def copy_to(peer, src):
        return pltpu.make_async_remote_copy(
            src_ref=send.at[peer], dst_ref=recv_ref.at[src], send_sem=sends.at[peer], recv_sem=recvs.at[src],
            device_id={"seq": peer}, device_id_type=MESH,
        )

    def pair(step, carry):
        first = lax.rem(me // 2 + 1 + step, n // 2)
        block = w_ref[:, pl.ds(pl.multiple_of(first * 256, 256), 256)]
        out = jnp.dot(x_ref[...], block, preferred_element_type=jnp.float32).astype(jnp.bfloat16).T
        for e in range(2):
            head = first * 2 + e
            gate_ref[head] = out[e * 128:e * 128 + 32]
            send[head] = out[e * 128 + 32:e * 128 + 128]

            @pl.when(head != me)
            def _():
                copy_to(head, me).start()
        return carry

    lax.fori_loop(0, n // 2, pair, 0)
    own = pltpu.make_async_copy(send.at[me], recv_ref.at[me], lsem)
    own.start()
    own.wait()

    def finish(step, carry):
        source = lax.rem(me + n - step, n)
        peer = lax.rem(me + step, n)
        count_copy(step, me).wait_send()
        copy_to(peer, me).wait_send()
        count_copy(step, source).wait_recv()
        copy_to(peer, source).wait_recv()
        return carry

    lax.fori_loop(1, n, finish, 0)


def project(embedded, weight, count, n):
    tokens, width = embedded.shape
    bf = jnp.bfloat16
    vm = pl.BlockSpec(memory_space=pltpu.VMEM)
    hbm = pl.BlockSpec(memory_space=pl.ANY)
    return pl.pallas_call(
        functools.partial(project_kernel, n),
        out_shape=(
            jax.ShapeDtypeStruct((n, 32, tokens), bf),
            jax.ShapeDtypeStruct((n, 96, tokens), bf),
            jax.ShapeDtypeStruct((n, 8, 128), jnp.int32),
        ),
        in_specs=[vm, hbm, vm],
        out_specs=(vm, hbm, vm),
        scratch_shapes=[
            pltpu.VMEM(weight.shape, bf),
            pltpu.VMEM((tokens, width), bf),
            pltpu.VMEM((n, 96, tokens), bf),
            pltpu.SemaphoreType.DMA((n,)),
            pltpu.SemaphoreType.DMA((n,)),
            pltpu.SemaphoreType.DMA((n,)),
            pltpu.SemaphoreType.DMA((n,)),
            pltpu.SemaphoreType.DMA,
            pltpu.SemaphoreType.DMA,
        ],
        compiler_params=pltpu.CompilerParams(collective_id=1, has_side_effects=True, vmem_limit_bytes=40 << 20),
        name="project",
    )(embedded, weight, count)


def finish_kernel(n, att_ref, gate_ref, emb_ref, wo_hbm, up_hbm, down_hbm, out_ref, back, wo, up, down, sends, recvs, wsems, lsem):
    me = lax.axis_index("seq")
    loads = [
        pltpu.make_async_copy(wo_hbm, wo, wsems.at[0]),
        pltpu.make_async_copy(up_hbm, up, wsems.at[1]),
        pltpu.make_async_copy(down_hbm, down, wsems.at[2]),
    ]
    for load in loads:
        load.start()
    greet(n)

    def copy_to(peer, src):
        return pltpu.make_async_remote_copy(
            src_ref=att_ref.at[peer], dst_ref=back.at[src], send_sem=sends.at[peer], recv_sem=recvs.at[src],
            device_id={"seq": peer}, device_id_type=MESH,
        )

    def begin(step, carry):
        copy_to(lax.rem(me + step, n), me).start()
        return carry

    lax.fori_loop(1, n, begin, 0)
    back[me] = att_ref[me]
    for load in loads:
        load.wait()

    def finish(step, carry):
        source = lax.rem(me + n - step, n)
        peer = lax.rem(me + step, n)
        copy_to(peer, me).wait_send()
        copy_to(peer, source).wait_recv()
        return carry

    lax.fori_loop(1, n, finish, 0)
    rows = 128

    def tail(step, carry):
        span = pl.ds(pl.multiple_of(step * rows, rows), rows)
        att = back[:, :, span].reshape(n * 32, rows).astype(jnp.float32)
        gate = gate_ref[:, :, span].reshape(n * 32, rows).astype(jnp.float32)
        gate = gate / (1.0 + jnp.exp(-gate))
        scale = lax.rsqrt(jnp.mean(att * att, axis=0, keepdims=True) + epsilon)
        heads = (att * scale * gate).astype(jnp.bfloat16).T
        hidden = emb_ref[span, :].astype(jnp.float32) + jnp.dot(heads, wo[...], preferred_element_type=jnp.float32)
        normed = (hidden * lax.rsqrt(jnp.mean(hidden * hidden, axis=-1, keepdims=True) + epsilon)).astype(jnp.bfloat16)
        wide = jnp.dot(normed, up[...], preferred_element_type=jnp.float32)
        active = (wide / (1.0 + jnp.exp(-wide))).astype(jnp.bfloat16)
        out = hidden + jnp.dot(active, down[...], preferred_element_type=jnp.float32)
        out_ref[span, :] = out.astype(jnp.bfloat16)
        return carry

    lax.fori_loop(0, emb_ref.shape[0] // rows, tail, 0)


def finish_layer(attended, gate, embedded, wo, up, down, n):
    tokens, width = embedded.shape
    bf = jnp.bfloat16
    vm = pl.BlockSpec(memory_space=pltpu.VMEM)
    hbm = pl.BlockSpec(memory_space=pl.ANY)
    return pl.pallas_call(
        functools.partial(finish_kernel, n),
        out_shape=jax.ShapeDtypeStruct((tokens, width), bf),
        in_specs=[vm, vm, vm, hbm, hbm, hbm],
        out_specs=vm,
        scratch_shapes=[
            pltpu.VMEM((n, 32, tokens), bf),
            pltpu.VMEM(wo.shape, bf),
            pltpu.VMEM(up.shape, bf),
            pltpu.VMEM(down.shape, bf),
            pltpu.SemaphoreType.DMA((n,)),
            pltpu.SemaphoreType.DMA((n,)),
            pltpu.SemaphoreType.DMA((3,)),
            pltpu.SemaphoreType.DMA,
        ],
        compiler_params=pltpu.CompilerParams(collective_id=2, has_side_effects=True, vmem_limit_bytes=40 << 20),
        name="finish",
    )(attended, gate, embedded, wo, up, down)


def local(token_rows, segment_ids, requests, hot_table, cold_table, input_weight, output_weight, up_weight, down_weight):
    seq_devices = lax.axis_size("seq")
    all_devices = lax.axis_size("emb") * seq_devices
    capacity = requests.shape[2]
    hot_count, model_width = hot_table.shape
    tokens_here = token_rows.shape[1]
    head_width = model_width // H
    below = jnp.sum(segment_ids[0][None, :] < jnp.arange(1, 4, dtype=jnp.int32)[:, None], axis=1, dtype=jnp.int32)
    count = jnp.broadcast_to(jnp.pad(below, (0, 125))[None], (8, 128))
    fetched = lax.all_to_all(
        cold_table[lax.all_to_all(requests[0], ("emb", "seq"), split_axis=0, concat_axis=0, tiled=True)],
        ("emb", "seq"), split_axis=0, concat_axis=0, tiled=True,
    ).reshape(all_devices * capacity, model_width)
    item_ids = token_rows[0]
    is_hot = item_ids < hot_count
    hot_rows = hot_table[jnp.where(is_hot, item_ids, 0)]
    cold_rows = fetched[jnp.where(is_hot, 0, item_ids - hot_count)]
    embedded = jnp.where(is_hot[:, None], hot_rows, cold_rows)
    gate, triples, counts = project(embedded, input_weight, count, seq_devices)
    starts = jnp.sum(counts[:, 0, :4], axis=0, dtype=jnp.int32)
    attended = attention(starts, triples, 512, 512, 2, True)
    return finish_layer(attended, gate, embedded, output_weight, up_weight, down_weight, seq_devices)[None]


def solution(mesh):
    placed = (
        P("emb", "seq"), P("emb", "seq"), P(("emb", "seq"), None, None), P(), P(("emb", "seq"), None), P(), P(), P(), P(),
    )
    return jax.shard_map(local, mesh=mesh, in_specs=placed, out_specs=P("emb", "seq", None), check_vma=False)
```

```python
import functools

import jax
import jax.numpy as jnp
from jax import lax
from jax.experimental import pallas as pl
from jax.experimental.pallas import tpu as pltpu
from jax.sharding import PartitionSpec as P

epsilon = 1e-06

BIG = float(2 ** 30)

def attn_kernel(TQ, TK, U, BF, segs_ref, qkv_ref, out_ref, q_scr, k_scr, v_scr, m_scr, a_scr, acc_scr):
    nb, _, W = qkv_ref.shape
    L = nb * W
    NQ = L // TQ
    segments = segs_ref[...]
    s1, s2, s3 = [
        jnp.sum((segments < s).astype(jnp.float32)).astype(jnp.int32) for s in (1, 2, 3)
    ]
    C = 0.5 / (32.0 ** 0.5)
    bf = jnp.bfloat16

    def prep(b, _):
        base = b * W
        lane = lax.broadcasted_iota(jnp.int32, (16, W), 1) + base
        row = lax.broadcasted_iota(jnp.int32, (16, W), 0)
        seg = (lane >= s1).astype(jnp.int32) + (lane >= s2).astype(jnp.int32) + (lane >= s3).astype(jnp.int32)
        hot = (seg == row).astype(jnp.float32)
        q = qkv_ref[b, 32:64, :].astype(jnp.float32) * C
        qx = jnp.concatenate([q.astype(bf), hot.astype(bf)], axis=0)
        for c in range(W // 256):
            q_scr[b * (W // 256) + c] = qx[:, c * 256:(c + 1) * 256]
        bias = jnp.where(row < 4, (1.0 - hot) * (-BIG), 0.0)
        kx = jnp.concatenate([qkv_ref[b, 64:96, :].astype(jnp.float32), bias], axis=0)
        k_scr[pl.ds(base, W), :] = kx.T.astype(bf)
        v = qkv_ref[b, 0:32, :]
        for c in range(W // 256):
            v_scr[b * (W // 256) + c] = v[:, c * 256:(c + 1) * 256]
        return 0
    lax.fori_loop(0, nb, prep, 0)

    R = TQ // TK
    for r in range(R):
        t = lax.broadcasted_iota(jnp.int32, (TK, TQ), 0) + r * TK
        qq = lax.broadcasted_iota(jnp.int32, (TK, TQ), 1)
        m_scr[r] = (t <= qq).astype(jnp.float32).astype(bf)
    m_scr[R] = jnp.ones((TK, TQ), bf)
    m_scr[R + 1] = jnp.zeros((TK, TQ), bf)

    def lo_of(i):
        p0 = i * TQ
        st = jnp.where(p0 >= s3, s3, jnp.where(p0 >= s2, s2, jnp.where(p0 >= s1, s1, 0)))
        return st // TK

    def count(i, n):
        return n + (i * R + R - lo_of(i))
    total = lax.fori_loop(0, NQ, count, 0)
    steps = (total + U - 1) // U

    def nxt(i, j):
        last = j <= lo_of(i)
        i2 = jnp.where(last, i + 1, i)
        j2 = jnp.where(last, (i + 1) * R + R - 1, j - 1)
        return i2, j2

    qh = TQ // 256
    kh = TK // 256

    def make(slot, i, j, valid):
        d = j - i * R
        ms = jnp.where(valid, jnp.where(d >= 0, d, R), R + 1)
        k = k_scr[pl.ds(j * TK, TK), :]
        for c in range(qh):
            q = q_scr[i * qh + c]
            s = jnp.dot(k, q, preferred_element_type=jnp.float32)
            if BF:
                h = s.astype(bf)
                a = h + h * jnp.tanh(h)
            else:
                a = (s + s * jnp.tanh(s)).astype(bf)
            a = a * m_scr[ms, :, c * 256:(c + 1) * 256]
            a_scr[slot, :, c * 256:(c + 1) * 256] = a

    def consume(slot, i, j, valid):
        first = j == i * R + R - 1
        for c in range(qh):
            o = jnp.where(first, 0.0, acc_scr[:, c * 256:(c + 1) * 256])
            for t in range(kh):
                o = o + jnp.dot(v_scr[j * kh + t], a_scr[slot, t * 256:(t + 1) * 256, c * 256:(c + 1) * 256],
                                preferred_element_type=jnp.float32)
            acc_scr[:, c * 256:(c + 1) * 256] = o
            if TQ <= W:
                bi = i // (W // TQ)
                if W == TQ:
                    out_ref[bi, :, c * 256:(c + 1) * 256] = o.astype(bf)
                else:
                    off = pl.multiple_of((i % (W // TQ)) * TQ, 256)
                    out_ref[bi, :, pl.ds(off, 256)] = o.astype(bf)
            else:
                out_ref[i * (TQ // W) + (c * 256) // W, :, (c * 256) % W:(c * 256) % W + 256] = o.astype(bf)

    def seq(n0, i, j):
        out = []
        for u in range(U):
            valid = n0 + u < total
            ic = jnp.where(valid, i, 0)
            jc = jnp.where(valid, j, 0)
            out.append((i, j, valid))
            i, j = nxt(i, j)
        return out, i, j

    def clamp(i, j, valid):
        return jnp.minimum(i, NQ - 1), jnp.where(valid, j, 0)

    i0 = jnp.int32(0); j0 = jnp.int32(R - 1)
    lst, i1, j1 = seq(0, i0, j0)
    for u, (i, j, v) in enumerate(lst):
        ci, cj = clamp(i, j, v)
        make(u, ci, cj, v)

    def body(n, carry):
        i, j, ni, nj = carry
        lst, _, _ = seq(n * U, i, j)
        lst2, n2i, n2j = seq((n + 1) * U, ni, nj)
        for u in range(U):
            ci, cj = clamp(*lst[u])
            consume(u, ci, cj, lst[u][2])
        for u in range(U):
            ci, cj = clamp(*lst2[u])
            make(u, ci, cj, lst2[u][2])
        return (ni, nj, n2i, n2j)
    lax.fori_loop(0, steps, body, (i0, j0, i1, j1))


def attention(segs, qkv, TQ=512, TK=512, U=1, BF=True):
    nb, _, W = qkv.shape
    L = nb * W
    bf = jnp.bfloat16
    R = TQ // TK
    return pl.pallas_call(
        functools.partial(attn_kernel, TQ, TK, U, BF),
        out_shape=jax.ShapeDtypeStruct((nb, 32, W), bf),
        in_specs=[pl.BlockSpec(memory_space=pltpu.VMEM), pl.BlockSpec(memory_space=pltpu.VMEM)],
        out_specs=pl.BlockSpec(memory_space=pltpu.VMEM),
        scratch_shapes=[
            pltpu.VMEM((L // 256, 48, 256), bf),
            pltpu.VMEM((L, 48), bf),
            pltpu.VMEM((L // 256, 32, 256), bf),
            pltpu.VMEM((R + 2, TK, TQ), bf),
            pltpu.VMEM((U, TK, TQ), bf),
            pltpu.VMEM((32, TQ), jnp.float32),
        ],
        compiler_params=pltpu.CompilerParams(vmem_limit_bytes=60 << 20),
        name="attn",
    )(segs, qkv)


MESH = pl.DeviceIdType.MESH


def one_hot(ids, base, width):
    lane = lax.broadcasted_iota(jnp.int32, ids.shape, 1).astype(jnp.float32)
    pieces = [
        jnp.where(ids == lane + (base + 128 * c), 1.0, 0.0).astype(jnp.bfloat16) for c in range(width // 128)
    ]
    return jnp.concatenate(pieces, axis=1)


def front_kernel(
    n, m, tok_ref, seg_ref, req_ref, hot_hbm, cold_hbm, w_hbm, emb_ref, gate_ref, recv_ref, segs_ref,
    hot, cold, w_ref, x_ref, send, asks, asked, rows_out, rows_in, acc, gat, tokb, idx, flat,
    sends, recvs, msems, lsems,
):
    me_s = lax.axis_index("seq")
    me = lax.axis_index("emb") * n + me_s
    total = n * m
    bf = jnp.bfloat16
    f32 = jnp.float32
    hot_count = hot_hbm.shape[0]
    cold_count = cold_hbm.shape[0]
    step_rows = 512

    barrier = pltpu.get_barrier_semaphore()

    def device(peer):
        return {"emb": peer // n, "seq": lax.rem(peer, n)}

    def signal(step, carry):
        peer = lax.rem(me + step, total)
        pl.semaphore_signal(barrier, inc=1, device_id=device(peer), device_id_type=MESH)
        return carry

    lax.fori_loop(1, total, signal, 0)
    hot_load = pltpu.make_async_copy(hot_hbm, hot, lsems.at[0])
    cold_load = pltpu.make_async_copy(cold_hbm, cold, lsems.at[1])
    w_load = pltpu.make_async_copy(w_hbm, w_ref, lsems.at[2])
    hot_load.start()
    cold_load.start()
    w_load.start()
    wanted = req_ref[0].astype(f32)
    wanted = jnp.concatenate([wanted, jnp.zeros((total - wanted.shape[0], total), f32)], axis=0).T
    asks[...] = wanted.reshape(total, 1, total)
    tokb[...] = jnp.broadcast_to(tok_ref[...].astype(f32), (128, tok_ref.shape[1])).T
    pl.semaphore_wait(barrier, total - 1)

    def ask(peer, src):
        return pltpu.make_async_remote_copy(
            src_ref=asks.at[peer], dst_ref=asked.at[src], send_sem=msems.at[0], recv_sem=msems.at[1],
            device_id=device(peer), device_id_type=MESH,
        )

    def start_ask(step, carry):
        ask(lax.rem(me + step, total), me).start()
        return carry

    lax.fori_loop(1, total, start_ask, 0)

    def seg_copy(step, src):
        return pltpu.make_async_remote_copy(
            src_ref=seg_ref, dst_ref=segs_ref.at[src], send_sem=msems.at[4], recv_sem=recvs.at[n + src],
            device_id={"seq": lax.rem(me_s + step, n)}, device_id_type=MESH,
        )

    asked[me] = asks[me]
    segs_ref[me_s] = seg_ref[...]

    hot_load.wait()
    acc[...] = jnp.zeros_like(acc)

    def add_hot(step, carry):
        base = step * step_rows
        pick = one_hot(tokb[...], base.astype(f32), step_rows)
        block = hot[pl.ds(pl.multiple_of(base, step_rows), step_rows), :]
        acc[...] += jnp.dot(pick, block, preferred_element_type=f32)
        return carry

    lax.fori_loop(0, hot_count // step_rows, add_hot, 0)

    every = pl.ds(0, total - 1)

    def all_of(src, dst, a, b):
        return pltpu.make_async_remote_copy(
            src_ref=src.at[every], dst_ref=dst.at[every], send_sem=msems.at[a], recv_sem=msems.at[b],
            device_id=device(me), device_id_type=MESH,
        )

    all_of(asks, asked, 0, 1).wait_recv()
    ids = asked[...].reshape(total, 128)
    high = jnp.floor(ids * (1.0 / 64.0))
    low = ids - high * 64.0
    slots = idx.shape[0]
    slot = lax.broadcasted_iota(jnp.int32, (slots, 128), 0)
    lane = lax.broadcasted_iota(jnp.int32, (slots, 128), 1)
    spread = jnp.where(slot // 4 == lane, 1.0, 0.0).astype(bf)
    ids = 64.0 * jnp.dot(spread, high.astype(bf), preferred_element_type=f32) + jnp.dot(
        spread, low.astype(bf), preferred_element_type=f32
    )
    ids = jnp.sum(jnp.where(lax.rem(slot, 4) == lane, ids, 0.0), axis=1, keepdims=True)
    idx[...] = jnp.broadcast_to(ids, (slots, 128))
    cold_load.wait()

    def give(peer, src):
        return pltpu.make_async_remote_copy(
            src_ref=rows_out.at[peer], dst_ref=rows_in.at[src], send_sem=msems.at[2], recv_sem=msems.at[3],
            device_id=device(peer), device_id_type=MESH,
        )

    half = slots // 2

    def serve(part, carry):
        gat[...] = jnp.zeros_like(gat)
        mine = idx[pl.ds(pl.multiple_of(part * half, half), half), :]

        def add_cold(step, inner):
            base = step * step_rows
            pick = one_hot(mine, base.astype(f32), step_rows)
            block = cold[pl.ds(pl.multiple_of(base, step_rows), step_rows), :]
            gat[...] += jnp.dot(pick, block, preferred_element_type=f32)
            return inner

        lax.fori_loop(0, cold_count // step_rows, add_cold, 0)
        rows_out[pl.ds(part * (total // 2), total // 2)] = gat[...].astype(bf).reshape(total // 2, 4, gat.shape[1])

        def start_give(step, inner):
            peer = part * (total // 2) + lax.rem(me + step, total // 2)

            @pl.when(peer != me)
            def _():
                give(peer, me).start()
            return inner

        lax.fori_loop(0, total // 2, start_give, 0)
        return carry

    lax.fori_loop(0, 2, serve, 0)
    rows_in[me] = rows_out[me]
    all_of(asks, asked, 0, 1).wait_send()

    def start_seg(step, carry):
        seg_copy(step, me_s).start()
        return carry

    lax.fori_loop(1, n, start_seg, 0)
    all_of(rows_out, rows_in, 2, 3).wait_recv()
    flat[...] = rows_in[...].reshape(flat.shape)
    pick = one_hot(tokb[...], float(hot_count), slots)
    found = (acc[...] + jnp.dot(pick, flat[...], preferred_element_type=f32)).astype(bf)
    emb_ref[...] = found
    x = found.astype(f32)
    x_ref[...] = (x * lax.rsqrt(jnp.mean(x * x, axis=-1, keepdims=True) + epsilon)).astype(bf)
    w_load.wait()

    def copy_to(peer, src):
        return pltpu.make_async_remote_copy(
            src_ref=send.at[peer], dst_ref=recv_ref.at[src], send_sem=sends.at[peer], recv_sem=recvs.at[src],
            device_id={"seq": peer}, device_id_type=MESH,
        )

    def pair(step, carry):
        first = lax.rem(me_s // 2 + 1 + step, n // 2)
        block = w_ref[:, pl.ds(pl.multiple_of(first * 256, 256), 256)]
        out = jnp.dot(x_ref[...], block, preferred_element_type=f32).astype(bf).T
        for e in range(2):
            head = first * 2 + e
            gate_ref[head] = out[e * 128:e * 128 + 32]
            send[head] = out[e * 128 + 32:e * 128 + 128]

            @pl.when(head != me_s)
            def _():
                copy_to(head, me_s).start()
        return carry

    lax.fori_loop(0, n // 2, pair, 0)
    own = pltpu.make_async_copy(send.at[me_s], recv_ref.at[me_s], lsems.at[3])
    own.start()
    all_of(rows_out, rows_in, 2, 3).wait_send()
    own.wait()

    def finish(step, carry):
        source = lax.rem(me_s + n - step, n)
        peer = lax.rem(me_s + step, n)
        copy_to(peer, me_s).wait_send()
        seg_copy(step, source).wait_recv()
        copy_to(peer, source).wait_recv()
        return carry

    lax.fori_loop(1, n, finish, 0)
    pltpu.make_async_remote_copy(
        src_ref=segs_ref.at[pl.ds(0, n - 1)], dst_ref=segs_ref.at[pl.ds(0, n - 1)], send_sem=msems.at[4],
        recv_sem=msems.at[4], device_id=device(me), device_id_type=MESH,
    ).wait_send()


def front(token_rows, segment_ids, requests, hot_table, cold_table, weight, n, m):
    tokens = token_rows.shape[1]
    width = hot_table.shape[1]
    total = n * m
    slots = total * requests.shape[1]
    bf = jnp.bfloat16
    f32 = jnp.float32
    vm = pl.BlockSpec(memory_space=pltpu.VMEM)
    hbm = pl.BlockSpec(memory_space=pltpu.HBM)
    return pl.pallas_call(
        functools.partial(front_kernel, n, m),
        out_shape=(
            jax.ShapeDtypeStruct((tokens, width), bf),
            jax.ShapeDtypeStruct((n, 32, tokens), bf),
            jax.ShapeDtypeStruct((n, 96, tokens), bf),
            jax.ShapeDtypeStruct((n, 1, tokens), jnp.int32),
        ),
        in_specs=[vm, vm, vm, hbm, hbm, hbm],
        out_specs=(vm, vm, hbm, vm),
        scratch_shapes=[
            pltpu.VMEM(hot_table.shape, bf),
            pltpu.VMEM(cold_table.shape, bf),
            pltpu.VMEM(weight.shape, bf),
            pltpu.VMEM((tokens, width), bf),
            pltpu.VMEM((n, 96, tokens), bf),
            pltpu.VMEM((total, 1, 128), f32),
            pltpu.VMEM((total, 1, 128), f32),
            pltpu.VMEM((total, 4, width), bf),
            pltpu.VMEM((total, 4, width), bf),
            pltpu.VMEM((tokens, width), f32),
            pltpu.VMEM((slots // 2, width), f32),
            pltpu.VMEM((tokens, 128), f32),
            pltpu.VMEM((slots, 128), f32),
            pltpu.VMEM((slots, width), bf),
            pltpu.SemaphoreType.DMA((n,)),
            pltpu.SemaphoreType.DMA((2 * n,)),
            pltpu.SemaphoreType.DMA((5,)),
            pltpu.SemaphoreType.DMA((4,)),
        ],
        compiler_params=pltpu.CompilerParams(collective_id=1, has_side_effects=True, vmem_limit_bytes=50 << 20),
        name="front",
    )(token_rows, segment_ids, requests, hot_table, cold_table, weight)


def greet(axis_size):
    me = lax.axis_index("seq")
    barrier = pltpu.get_barrier_semaphore()

    def signal(step, carry):
        peer = lax.rem(me + step, axis_size)
        pl.semaphore_signal(barrier, inc=1, device_id={"seq": peer}, device_id_type=MESH)
        return carry

    lax.fori_loop(1, axis_size, signal, 0)
    pl.semaphore_wait(barrier, axis_size - 1)


def finish_kernel(n, att_ref, gate_ref, emb_ref, wo_hbm, up_hbm, down_hbm, out_ref, back, wo, up, down, sends, recvs, wsems, lsem):
    me = lax.axis_index("seq")
    loads = [
        pltpu.make_async_copy(wo_hbm, wo, wsems.at[0]),
        pltpu.make_async_copy(up_hbm, up, wsems.at[1]),
        pltpu.make_async_copy(down_hbm, down, wsems.at[2]),
    ]
    for load in loads:
        load.start()
    greet(n)

    def copy_to(peer, src):
        return pltpu.make_async_remote_copy(
            src_ref=att_ref.at[peer], dst_ref=back.at[src], send_sem=sends.at[peer], recv_sem=recvs.at[src],
            device_id={"seq": peer}, device_id_type=MESH,
        )

    def begin(step, carry):
        copy_to(lax.rem(me + step, n), me).start()
        return carry

    lax.fori_loop(1, n, begin, 0)
    back[me] = att_ref[me]
    for load in loads:
        load.wait()

    def finish(step, carry):
        source = lax.rem(me + n - step, n)
        peer = lax.rem(me + step, n)
        copy_to(peer, me).wait_send()
        copy_to(peer, source).wait_recv()
        return carry

    lax.fori_loop(1, n, finish, 0)
    rows = 128

    def tail(step, carry):
        span = pl.ds(pl.multiple_of(step * rows, rows), rows)
        att = back[:, :, span].reshape(n * 32, rows).astype(jnp.float32)
        gate = gate_ref[:, :, span].reshape(n * 32, rows).astype(jnp.float32)
        gate = gate / (1.0 + jnp.exp(-gate))
        scale = lax.rsqrt(jnp.mean(att * att, axis=0, keepdims=True) + epsilon)
        heads = (att * scale * gate).astype(jnp.bfloat16).T
        hidden = emb_ref[span, :].astype(jnp.float32) + jnp.dot(heads, wo[...], preferred_element_type=jnp.float32)
        normed = (hidden * lax.rsqrt(jnp.mean(hidden * hidden, axis=-1, keepdims=True) + epsilon)).astype(jnp.bfloat16)
        wide = jnp.dot(normed, up[...], preferred_element_type=jnp.float32)
        active = (wide / (1.0 + jnp.exp(-wide))).astype(jnp.bfloat16)
        out = hidden + jnp.dot(active, down[...], preferred_element_type=jnp.float32)
        out_ref[span, :] = out.astype(jnp.bfloat16)
        return carry

    lax.fori_loop(0, emb_ref.shape[0] // rows, tail, 0)


def finish_layer(attended, gate, embedded, wo, up, down, n):
    tokens, width = embedded.shape
    bf = jnp.bfloat16
    vm = pl.BlockSpec(memory_space=pltpu.VMEM)
    hbm = pl.BlockSpec(memory_space=pltpu.HBM)
    return pl.pallas_call(
        functools.partial(finish_kernel, n),
        out_shape=jax.ShapeDtypeStruct((tokens, width), bf),
        in_specs=[vm, vm, vm, hbm, hbm, hbm],
        out_specs=vm,
        scratch_shapes=[
            pltpu.VMEM((n, 32, tokens), bf),
            pltpu.VMEM(wo.shape, bf),
            pltpu.VMEM(up.shape, bf),
            pltpu.VMEM(down.shape, bf),
            pltpu.SemaphoreType.DMA((n,)),
            pltpu.SemaphoreType.DMA((n,)),
            pltpu.SemaphoreType.DMA((3,)),
            pltpu.SemaphoreType.DMA,
        ],
        compiler_params=pltpu.CompilerParams(collective_id=2, has_side_effects=True, vmem_limit_bytes=40 << 20),
        name="finish",
    )(attended, gate, embedded, wo, up, down)


def local(token_rows, segment_ids, requests, hot_table, cold_table, input_weight, output_weight, up_weight, down_weight):
    n = lax.axis_size("seq")
    m = lax.axis_size("emb")
    embedded, gate, triples, segments = front(
        token_rows, segment_ids, jnp.transpose(requests, (0, 2, 1)), hot_table, cold_table, input_weight, n, m
    )
    attended = attention(segments, triples, 512, 512, 2, True)
    return finish_layer(attended, gate, embedded, output_weight, up_weight, down_weight, n)[None]


def solution(mesh):
    placed = (
        P("emb", "seq"), P("emb", "seq"), P(("emb", "seq"), None, None), P(), P(("emb", "seq"), None), P(), P(), P(), P(),
    )
    return jax.shard_map(local, mesh=mesh, in_specs=placed, out_specs=P("emb", "seq", None), check_vma=False)
```

```python
import functools

import jax
import jax.numpy as jnp
from jax import lax
from jax.experimental import pallas as pl
from jax.experimental.pallas import tpu as pltpu
from jax.sharding import PartitionSpec as P

epsilon = 1e-06

BIG = float(2 ** 30)


def attn_kernel(U, seg_ref, qkv_ref, out_ref, q_scr, k_scr, m_scr, a_scr, acc_scr):
    blocks, _, W = qkv_ref.shape
    bf = jnp.bfloat16
    f32 = jnp.float32
    segments = seg_ref[...]
    s1, s2, s3 = [jnp.sum((segments < s).astype(f32)).astype(jnp.int32) for s in (1, 2, 3)]
    scale = 0.5 / (32.0 ** 0.5)

    def prep(b, carry):
        base = b * W
        lane = lax.broadcasted_iota(jnp.int32, (16, W), 1) + base
        row = lax.broadcasted_iota(jnp.int32, (16, W), 0)
        seg = (lane >= s1).astype(jnp.int32) + (lane >= s2).astype(jnp.int32) + (lane >= s3).astype(jnp.int32)
        same = (seg == row).astype(f32)
        q_scr[b, 0:32] = (qkv_ref[b, 32:64, :].astype(f32) * scale).astype(bf)
        q_scr[b, 32:48] = same.astype(bf)
        bias = jnp.where(row < 4, (1.0 - same) * (-BIG), 0.0).astype(bf)
        k_scr[pl.ds(base, W), :] = jnp.concatenate([qkv_ref[b, 64:96, :], bias], axis=0).T
        return carry

    lax.fori_loop(0, blocks, prep, 0, unroll=2)
    t = lax.broadcasted_iota(jnp.int32, (W, W), 0)
    p = lax.broadcasted_iota(jnp.int32, (W, W), 1)
    m_scr[0] = (t <= p).astype(f32).astype(bf)
    m_scr[1] = jnp.ones((W, W), bf)
    m_scr[2] = jnp.zeros((W, W), bf)

    def low(i):
        first = i * W
        start = jnp.where(first >= s3, s3, jnp.where(first >= s2, s2, jnp.where(first >= s1, s1, 0)))
        return start // W

    total = lax.fori_loop(0, blocks, lambda i, c: c + (i + 1 - low(i)), 0)

    def after(i, j):
        last = j <= low(i)
        return jnp.where(last, i + 1, i), jnp.where(last, i + 1, j - 1)

    def weigh(slot, i, j, valid):
        kind = jnp.where(valid, jnp.where(j == i, 0, 1), 2)
        i = jnp.minimum(i, blocks - 1)
        j = jnp.where(valid, j, 0)
        k = k_scr[pl.ds(pl.multiple_of(j * W, W), W), :]
        s = jnp.dot(k, q_scr[i], preferred_element_type=f32)
        h = s.astype(bf)
        a_scr[slot] = (h + h * jnp.tanh(h)) * m_scr[kind]

    def gather(slot, i, j, valid):
        i = jnp.minimum(i, blocks - 1)
        j = jnp.where(valid, j, 0)
        first = valid & (i == j)
        o = jnp.where(first, 0.0, acc_scr[...])
        o = o + jnp.dot(qkv_ref[j, 0:32, :], a_scr[slot], preferred_element_type=f32)
        acc_scr[...] = o
        out_ref[i] = o.astype(bf)

    def some(n, i, j):
        out = []
        for u in range(U):
            out.append((i, j, n * U + u < total))
            i, j = after(i, j)
        return out, i, j

    zero = jnp.int32(0)
    head, i1, j1 = some(0, zero, zero)
    for u in range(U):
        weigh(u, *head[u])

    def body(n, carry):
        i, j, ni, nj = carry
        now, _, _ = some(n, i, j)
        then, mi, mj = some(n + 1, ni, nj)
        for u in range(U):
            gather(u, *now[u])
            weigh(u, *then[u])
        return ni, nj, mi, mj

    lax.fori_loop(0, (total + U - 1) // U, body, (zero, zero, i1, j1))


def attention(segs, qkv, U):
    blocks, _, W = qkv.shape
    bf = jnp.bfloat16
    vm = pl.BlockSpec(memory_space=pltpu.VMEM)
    return pl.pallas_call(
        functools.partial(attn_kernel, U),
        out_shape=jax.ShapeDtypeStruct((blocks, 32, W), bf),
        in_specs=[vm, vm],
        out_specs=vm,
        scratch_shapes=[
            pltpu.VMEM((blocks, 48, W), bf),
            pltpu.VMEM((blocks * W, 48), bf),
            pltpu.VMEM((3, W, W), bf),
            pltpu.VMEM((U, W, W), bf),
            pltpu.VMEM((32, W), jnp.float32),
        ],
        compiler_params=pltpu.CompilerParams(vmem_limit_bytes=16 << 20),
        name="attn",
    )(segs, qkv)


MESH = pl.DeviceIdType.MESH


def one_hot(ids, base, width):
    lane = lax.broadcasted_iota(jnp.int32, ids.shape, 1).astype(jnp.float32)
    pieces = [
        jnp.where(ids == lane + (base + 128 * c), 1.0, 0.0).astype(jnp.bfloat16) for c in range(width // 128)
    ]
    return jnp.concatenate(pieces, axis=1)


def front_kernel(
    n, m, tok_hbm, seg_hbm, req_hbm, hot_hbm, cold_hbm, w_hbm, emb_ref, gate_ref, recv_ref, segs_ref,
    tok_ref, seg_ref, req_ref, hot, cold, w_ref, x_ref, send, asks, asked, rows_out, rows_in, acc, gat, tokb, idx, flat,
    sends, recvs, msems, lsems,
):
    me_s = lax.axis_index("seq")
    me = lax.axis_index("emb") * n + me_s
    total = n * m
    bf = jnp.bfloat16
    f32 = jnp.float32
    hot_count = hot_hbm.shape[0]
    cold_count = cold_hbm.shape[0]
    hot_rows, cold_rows = 1024, 2048
    side = 4
    me_z, me_y = me_s // side, lax.rem(me_s, side)
    me_x = lax.axis_index("emb") // 2
    far = (2, 1, 3, 0)

    barrier = pltpu.get_barrier_semaphore()

    def device(peer):
        return {"emb": peer // n, "seq": lax.rem(peer, n)}

    def signal(step, carry):
        peer = lax.rem(me + step, total)
        pl.semaphore_signal(barrier, inc=1, device_id=device(peer), device_id_type=MESH)
        return carry

    small = [
        pltpu.make_async_copy(a, b, lsems.at[4 + c])
        for c, (a, b) in enumerate(((tok_hbm, tok_ref), (req_hbm, req_ref), (seg_hbm, seg_ref)))
    ]
    for load in small:
        load.start()
    lax.fori_loop(1, total, signal, 0)
    hot_load = pltpu.make_async_copy(hot_hbm, hot, lsems.at[0])
    cold_load = pltpu.make_async_copy(cold_hbm, cold, lsems.at[1])
    w_load = pltpu.make_async_copy(w_hbm, w_ref, lsems.at[2])
    hot_load.start()
    cold_load.start()
    w_load.start()
    for load in small:
        load.wait()
    wanted = req_ref[0].astype(f32)
    wanted = jnp.concatenate([wanted, jnp.zeros((total - wanted.shape[0], total), f32)], axis=0).T
    asks[...] = wanted.reshape(total, 1, total)
    tokb[...] = jnp.broadcast_to(tok_ref[...].astype(f32), (128, tok_ref.shape[1])).T
    pl.semaphore_wait(barrier, total - 1)

    def ask(peer, src):
        return pltpu.make_async_remote_copy(
            src_ref=asks.at[peer], dst_ref=asked.at[src], send_sem=msems.at[0], recv_sem=msems.at[1],
            device_id=device(peer), device_id_type=MESH,
        )

    def away(step):
        return lax.rem(me_z + 2 + step // side, side) * side + lax.rem(me_y + 2 + step, side)

    def peer_at(dx, core, step):
        return (lax.rem(me_x + dx, side) * 2 + core) * n + away(step)

    def start_ask(step, carry):
        for dx in far:
            for core in range(2):
                peer = peer_at(dx, core, step)

                @pl.when(peer != me)
                def _():
                    ask(peer, me).start()
        return carry

    lax.fori_loop(0, n, start_ask, 0)

    def seg_copy(step, src):
        return pltpu.make_async_remote_copy(
            src_ref=seg_ref, dst_ref=segs_ref.at[src], send_sem=msems.at[4], recv_sem=recvs.at[n + src],
            device_id={"seq": lax.rem(me_s + step, n)}, device_id_type=MESH,
        )

    def start_seg(step, carry):
        seg_copy(step, me_s).start()
        return carry

    lax.fori_loop(1, n, start_seg, 0)
    asked[me] = asks[me]
    segs_ref[me_s] = seg_ref[...]

    hot_load.wait()
    acc[...] = jnp.zeros_like(acc)

    def add_hot(step, carry):
        base = step * hot_rows
        pick = one_hot(tokb[...], base.astype(f32), hot_rows)
        block = hot[pl.ds(pl.multiple_of(base, hot_rows), hot_rows), :]
        acc[...] += jnp.dot(pick, block, preferred_element_type=f32)
        return carry

    lax.fori_loop(0, hot_count // hot_rows, add_hot, 0)

    every = pl.ds(0, total - 1)

    def all_of(src, dst, a, b):
        return pltpu.make_async_remote_copy(
            src_ref=src.at[every], dst_ref=dst.at[every], send_sem=msems.at[a], recv_sem=msems.at[b],
            device_id=device(me), device_id_type=MESH,
        )

    all_of(asks, asked, 0, 1).wait_recv()
    ids = asked[...].reshape(total, 128)
    high = jnp.floor(ids * (1.0 / 64.0))
    low = ids - high * 64.0
    slots = idx.shape[0]
    slot = lax.broadcasted_iota(jnp.int32, (slots, 128), 0)
    lane = lax.broadcasted_iota(jnp.int32, (slots, 128), 1)
    spread = jnp.where(slot // 4 == lane, 1.0, 0.0).astype(bf)
    ids = 64.0 * jnp.dot(spread, high.astype(bf), preferred_element_type=f32) + jnp.dot(
        spread, low.astype(bf), preferred_element_type=f32
    )
    ids = jnp.sum(jnp.where(lax.rem(slot, 4) == lane, ids, 0.0), axis=1, keepdims=True)
    idx[...] = jnp.broadcast_to(ids, (slots, 128))
    cold_load.wait()

    def give(peer, src):
        return pltpu.make_async_remote_copy(
            src_ref=rows_out.at[peer], dst_ref=rows_in.at[src], send_sem=msems.at[2], recv_sem=msems.at[3],
            device_id=device(peer), device_id_type=MESH,
        )

    def serve(first, second):
        gat[...] = jnp.zeros_like(gat)
        group = total // side
        spans = [lax.rem(me_x + dx, side) for dx in (first, second)]
        mine = jnp.concatenate(
            [idx[pl.ds(pl.multiple_of(x * group * 4, group * 4), group * 4), :] for x in spans], axis=0
        )

        def add_cold(step, inner):
            base = step * cold_rows
            pick = one_hot(mine, base.astype(f32), cold_rows)
            block = cold[pl.ds(pl.multiple_of(base, cold_rows), cold_rows), :]
            gat[...] += jnp.dot(pick, block, preferred_element_type=f32)
            return inner

        lax.fori_loop(0, cold_count // cold_rows, add_cold, 0)
        for c, x in enumerate(spans):
            part = gat[c * group * 4:(c + 1) * group * 4, :].astype(bf)
            rows_out[pl.ds(x * group, group)] = part.reshape(group, 4, part.shape[1])

        def start_give(step, inner):
            for dx in (first, second):
                for core in range(2):
                    peer = peer_at(dx, core, step)

                    @pl.when(peer != me)
                    def _():
                        give(peer, me).start()
            return inner

        lax.fori_loop(0, n, start_give, 0)

    serve(2, 1)
    serve(3, 0)
    rows_in[me] = rows_out[me]
    all_of(asks, asked, 0, 1).wait_send()

    all_of(rows_out, rows_in, 2, 3).wait_recv()
    flat[...] = rows_in[...].reshape(flat.shape)
    pick = one_hot(tokb[...], float(hot_count), slots)
    found = (acc[...] + jnp.dot(pick, flat[...], preferred_element_type=f32)).astype(bf)
    emb_ref[...] = found
    x = found.astype(f32)
    x_ref[...] = (x * lax.rsqrt(jnp.mean(x * x, axis=-1, keepdims=True) + epsilon)).astype(bf)
    w_load.wait()

    def copy_to(peer, src):
        return pltpu.make_async_remote_copy(
            src_ref=send.at[peer], dst_ref=recv_ref.at[src], send_sem=sends.at[peer], recv_sem=recvs.at[src],
            device_id={"seq": peer}, device_id_type=MESH,
        )

    for dz in far:
        z = lax.rem(me_z + dz, side)
        block = w_ref[:, pl.ds(pl.multiple_of(z * 512, 512), 512)]
        out = jnp.dot(x_ref[...], block, preferred_element_type=f32).astype(bf).T
        for y in range(side):
            gate_ref[z * side + y] = out[y * 128:y * 128 + 32]
            send[z * side + y] = out[y * 128 + 32:y * 128 + 128]
        for dy in far:
            if (dz, dy) != (0, 0):
                copy_to(z * side + lax.rem(me_y + dy, side), me_s).start()
    recv_ref[me_s] = send[me_s]
    all_of(rows_out, rows_in, 2, 3).wait_send()

    def finish(step, carry):
        source = lax.rem(me_s + n - step, n)
        peer = lax.rem(me_s + step, n)
        copy_to(peer, me_s).wait_send()
        seg_copy(step, source).wait_recv()
        copy_to(peer, source).wait_recv()
        return carry

    lax.fori_loop(1, n, finish, 0)
    pltpu.make_async_remote_copy(
        src_ref=segs_ref.at[pl.ds(0, n - 1)], dst_ref=segs_ref.at[pl.ds(0, n - 1)], send_sem=msems.at[4],
        recv_sem=msems.at[4], device_id=device(me), device_id_type=MESH,
    ).wait_send()


def front(token_rows, segment_ids, requests, hot_table, cold_table, weight, n, m):
    tokens = token_rows.shape[1]
    width = hot_table.shape[1]
    total = n * m
    slots = total * requests.shape[1]
    bf = jnp.bfloat16
    f32 = jnp.float32
    vm = pl.BlockSpec(memory_space=pltpu.VMEM)
    hbm = pl.BlockSpec(memory_space=pltpu.HBM)
    return pl.pallas_call(
        functools.partial(front_kernel, n, m),
        out_shape=(
            jax.ShapeDtypeStruct((tokens, width), bf),
            jax.ShapeDtypeStruct((n, 32, tokens), bf),
            jax.ShapeDtypeStruct((n, 96, tokens), bf),
            jax.ShapeDtypeStruct((n, 1, tokens), jnp.int32),
        ),
        in_specs=[hbm] * 6,
        out_specs=(vm, vm, vm, vm),
        scratch_shapes=[
            pltpu.VMEM(token_rows.shape, jnp.int32),
            pltpu.VMEM(segment_ids.shape, jnp.int32),
            pltpu.VMEM(requests.shape, jnp.int32),
            pltpu.VMEM(hot_table.shape, bf),
            pltpu.VMEM(cold_table.shape, bf),
            pltpu.VMEM(weight.shape, bf),
            pltpu.VMEM((tokens, width), bf),
            pltpu.VMEM((n, 96, tokens), bf),
            pltpu.VMEM((total, 1, 128), f32),
            pltpu.VMEM((total, 1, 128), f32),
            pltpu.VMEM((total, 4, width), bf),
            pltpu.VMEM((total, 4, width), bf),
            pltpu.VMEM((tokens, width), f32),
            pltpu.VMEM((slots // 2, width), f32),
            pltpu.VMEM((tokens, 128), f32),
            pltpu.VMEM((slots, 128), f32),
            pltpu.VMEM((slots, width), bf),
            pltpu.SemaphoreType.DMA((n,)),
            pltpu.SemaphoreType.DMA((2 * n,)),
            pltpu.SemaphoreType.DMA((5,)),
            pltpu.SemaphoreType.DMA((7,)),
        ],
        compiler_params=pltpu.CompilerParams(collective_id=1, has_side_effects=True, vmem_limit_bytes=50 << 20),
        name="front",
    )(*[
        pltpu.with_memory_space_constraint(x, pltpu.HBM)
        for x in (token_rows, segment_ids, requests, hot_table, cold_table, weight)
    ])


def greet(axis_size):
    me = lax.axis_index("seq")
    barrier = pltpu.get_barrier_semaphore()

    def signal(step, carry):
        peer = lax.rem(me + step, axis_size)
        pl.semaphore_signal(barrier, inc=1, device_id={"seq": peer}, device_id_type=MESH)
        return carry

    lax.fori_loop(1, axis_size, signal, 0)
    pl.semaphore_wait(barrier, axis_size - 1)


def finish_kernel(n, att_ref, gate_ref, emb_ref, wo, up, down, out_ref, back, open_gate, sends, recvs):
    me = lax.axis_index("seq")
    greet(n)

    def copy_to(peer, src):
        return pltpu.make_async_remote_copy(
            src_ref=att_ref.at[peer], dst_ref=back.at[src], send_sem=sends.at[peer], recv_sem=recvs.at[src],
            device_id={"seq": peer}, device_id_type=MESH,
        )

    side = 4
    far = (2, 1, 3, 0)
    for dz in far:
        for dy in far:
            if (dz, dy) != (0, 0):
                peer = lax.rem(me // side + dz, side) * side + lax.rem(me + dy, side)
                copy_to(peer, me).start()
    back[me] = att_ref[me]

    def open_one(step, carry):
        gate = gate_ref[step].astype(jnp.float32)
        open_gate[step] = gate / (1.0 + jnp.exp(-gate))
        return carry

    lax.fori_loop(0, n, open_one, 0)

    def finish(step, carry):
        source = lax.rem(me + n - step, n)
        peer = lax.rem(me + step, n)
        copy_to(peer, me).wait_send()
        copy_to(peer, source).wait_recv()
        return carry

    lax.fori_loop(1, n, finish, 0)
    rows = 256

    def tail(step, carry):
        span = pl.ds(pl.multiple_of(step * rows, rows), rows)
        att = back[:, :, span].reshape(n * 32, rows).astype(jnp.float32)
        gate = open_gate[:, :, span].reshape(n * 32, rows)
        scale = lax.rsqrt(jnp.mean(att * att, axis=0, keepdims=True) + epsilon)
        heads = (att * scale * gate).astype(jnp.bfloat16).T
        hidden = emb_ref[span, :].astype(jnp.float32) + jnp.dot(heads, wo[...], preferred_element_type=jnp.float32)
        normed = (hidden * lax.rsqrt(jnp.mean(hidden * hidden, axis=-1, keepdims=True) + epsilon)).astype(jnp.bfloat16)
        wide = jnp.dot(normed, up[...], preferred_element_type=jnp.float32)
        active = (wide / (1.0 + jnp.exp(-wide))).astype(jnp.bfloat16)
        out = hidden + jnp.dot(active, down[...], preferred_element_type=jnp.float32)
        out_ref[span, :] = out.astype(jnp.bfloat16)
        return carry

    lax.fori_loop(0, emb_ref.shape[0] // rows, tail, 0)


def finish_layer(attended, gate, embedded, wo, up, down, n):
    tokens, width = embedded.shape
    bf = jnp.bfloat16
    vm = pl.BlockSpec(memory_space=pltpu.VMEM)
    return pl.pallas_call(
        functools.partial(finish_kernel, n),
        out_shape=jax.ShapeDtypeStruct((tokens, width), bf),
        in_specs=[vm] * 6,
        out_specs=vm,
        scratch_shapes=[
            pltpu.VMEM((n, 32, tokens), bf),
            pltpu.VMEM((n, 32, tokens), jnp.float32),
            pltpu.SemaphoreType.DMA((n,)),
            pltpu.SemaphoreType.DMA((n,)),
        ],
        compiler_params=pltpu.CompilerParams(collective_id=2, has_side_effects=True, vmem_limit_bytes=20 << 20),
        name="finish",
    )(attended, gate, embedded, wo, up, down)


def local(token_rows, segment_ids, requests, hot_table, cold_table, input_weight, output_weight, up_weight, down_weight):
    n = lax.axis_size("seq")
    m = lax.axis_size("emb")
    embedded, gate, triples, segments = front(
        token_rows, segment_ids, jnp.transpose(requests, (0, 2, 1)), hot_table, cold_table, input_weight, n, m
    )
    attended = attention(segments, triples, 4)
    return finish_layer(attended, gate, embedded, output_weight, up_weight, down_weight, n)[None]


def solution(mesh):
    placed = (
        P("emb", "seq"), P("emb", "seq"), P(("emb", "seq"), None, None), P(), P(("emb", "seq"), None), P(), P(), P(), P(),
    )
    return jax.shard_map(local, mesh=mesh, in_specs=placed, out_specs=P("emb", "seq", None), check_vma=False)
```

```python
import functools

import jax
import jax.numpy as jnp
from jax import lax
from jax.experimental import pallas as pl
from jax.experimental.pallas import tpu as pltpu
from jax.sharding import PartitionSpec as P

epsilon = 1e-06

BIG = float(2 ** 30)


def attn_kernel(U, seg_ref, qkv_ref, out_ref, q_scr, k_scr, m_scr, a_scr, acc_scr):
    blocks, _, W = qkv_ref.shape
    bf = jnp.bfloat16
    f32 = jnp.float32
    segments = seg_ref[:, 0:1, :]
    s1, s2, s3 = [jnp.sum((segments < s).astype(f32)).astype(jnp.int32) for s in (1, 2, 3)]
    scale = 0.5 / (32.0 ** 0.5)

    def prep(b, carry):
        base = b * W
        lane = lax.broadcasted_iota(jnp.int32, (16, W), 1) + base
        row = lax.broadcasted_iota(jnp.int32, (16, W), 0)
        seg = (lane >= s1).astype(jnp.int32) + (lane >= s2).astype(jnp.int32) + (lane >= s3).astype(jnp.int32)
        same = (seg == row).astype(f32)
        q_scr[b, 0:32] = (qkv_ref[b, 32:64, :].astype(f32) * scale).astype(bf)
        q_scr[b, 32:48] = same.astype(bf)
        bias = jnp.where(row < 4, (1.0 - same) * (-BIG), 0.0).astype(bf)
        k_scr[pl.ds(base, W), :] = jnp.concatenate([qkv_ref[b, 64:96, :], bias], axis=0).T
        return carry

    lax.fori_loop(0, blocks, prep, 0, unroll=2)
    t = lax.broadcasted_iota(jnp.int32, (W, W), 0)
    p = lax.broadcasted_iota(jnp.int32, (W, W), 1)
    m_scr[0] = (t <= p).astype(f32).astype(bf)
    m_scr[1] = jnp.ones((W, W), bf)
    m_scr[2] = jnp.zeros((W, W), bf)

    def low(i):
        first = i * W
        start = jnp.where(first >= s3, s3, jnp.where(first >= s2, s2, jnp.where(first >= s1, s1, 0)))
        return start // W

    total = lax.fori_loop(0, blocks, lambda i, c: c + (i + 1 - low(i)), 0)

    def after(i, j):
        last = j <= low(i)
        return jnp.where(last, i + 1, i), jnp.where(last, i + 1, j - 1)

    def weigh(slot, i, j, valid):
        kind = jnp.where(valid, jnp.where(j == i, 0, 1), 2)
        i = jnp.minimum(i, blocks - 1)
        j = jnp.where(valid, j, 0)
        k = k_scr[pl.ds(pl.multiple_of(j * W, W), W), :]
        s = jnp.dot(k, q_scr[i], preferred_element_type=f32)
        h = s.astype(bf)
        a_scr[slot] = (h + h * jnp.tanh(h)) * m_scr[kind]

    def gather(slot, i, j, valid):
        i = jnp.minimum(i, blocks - 1)
        j = jnp.where(valid, j, 0)
        first = valid & (i == j)
        o = jnp.where(first, 0.0, acc_scr[...])
        o = o + jnp.dot(qkv_ref[j, 0:32, :], a_scr[slot], preferred_element_type=f32)
        acc_scr[...] = o
        out_ref[i] = o.astype(bf)

    def some(n, i, j):
        out = []
        for u in range(U):
            out.append((i, j, n * U + u < total))
            i, j = after(i, j)
        return out, i, j

    zero = jnp.int32(0)
    head, i1, j1 = some(0, zero, zero)
    for u in range(U):
        weigh(u, *head[u])

    def body(n, carry):
        i, j, ni, nj = carry
        now, _, _ = some(n, i, j)
        then, mi, mj = some(n + 1, ni, nj)
        for u in range(U):
            gather(u, *now[u])
            weigh(u, *then[u])
        return ni, nj, mi, mj

    lax.fori_loop(0, (total + U - 1) // U, body, (zero, zero, i1, j1))


def attention(segs, qkv, U):
    blocks, _, W = qkv.shape
    bf = jnp.bfloat16
    vm = pl.BlockSpec(memory_space=pltpu.VMEM)
    return pl.pallas_call(
        functools.partial(attn_kernel, U),
        out_shape=jax.ShapeDtypeStruct((blocks, 32, W), bf),
        in_specs=[vm, vm],
        out_specs=vm,
        scratch_shapes=[
            pltpu.VMEM((blocks, 48, W), bf),
            pltpu.VMEM((blocks * W, 48), bf),
            pltpu.VMEM((3, W, W), bf),
            pltpu.VMEM((U, W, W), bf),
            pltpu.VMEM((32, W), jnp.float32),
        ],
        compiler_params=pltpu.CompilerParams(vmem_limit_bytes=16 << 20),
        name="attn",
    )(segs, qkv)


MESH = pl.DeviceIdType.MESH


def one_hot(ids, base, width):
    lane = lax.broadcasted_iota(jnp.int32, ids.shape, 1).astype(jnp.float32)
    pieces = [
        jnp.where(ids == lane + (base + 128 * c), 1.0, 0.0).astype(jnp.bfloat16) for c in range(width // 128)
    ]
    return jnp.concatenate(pieces, axis=1)


def normalize(values):
    x = values.astype(jnp.float32)
    return (x * lax.rsqrt(jnp.mean(x * x, axis=-1, keepdims=True) + epsilon)).astype(jnp.bfloat16)


def select_exact(pick, ids):
    high = jnp.floor(ids * (1.0 / 64.0))
    low = ids - high * 64.0
    return 64.0 * jnp.dot(pick, high.astype(jnp.bfloat16), preferred_element_type=jnp.float32) + jnp.dot(
        pick, low.astype(jnp.bfloat16), preferred_element_type=jnp.float32
    )


def front_kernel(
    n, m, tok_hbm, seg_hbm, req_hbm, hot_hbm, cold_hbm, w_hbm, emb_ref, gate_ref, qkv_ref, info_ref,
    tok_ref, seg_ref, req_ref, hot, cold, w_ref, send, recv, gates, emb_packed, info, asks, asked,
    rows_out, rows_in, gat, packed, rank_t, idx, flat, msems, crecvs, lsems,
):
    side = 4
    me_s = lax.axis_index("seq")
    me = lax.axis_index("emb") * n + me_s
    me_z, me_y = me_s // side, lax.rem(me_s, side)
    me_x = lax.axis_index("emb") // 2
    total = n * m
    bf = jnp.bfloat16
    f32 = jnp.float32
    hot_count = hot_hbm.shape[0]
    cold_count = cold_hbm.shape[0]
    tokens = tok_hbm.shape[1]
    half = tokens // 2
    slots = idx.shape[0]
    far = (2, 1, 3, 0)
    wide = 2048

    barrier = pltpu.get_barrier_semaphore()
    small = [
        pltpu.make_async_copy(a, b, lsems.at[3 + c])
        for c, (a, b) in enumerate(((tok_hbm, tok_ref), (req_hbm, req_ref), (seg_hbm, seg_ref)))
    ]
    for load in small:
        load.start()

    def device(peer):
        return {"emb": peer // n, "seq": lax.rem(peer, n)}

    def away(step):
        t = step // side
        u = lax.rem(step, side)
        dz = lax.rem(2 + 3 * t + 3 * (t // 2) + 2 * (t // 3), side)
        dy = lax.rem(2 + 3 * u + 3 * (u // 2) + 2 * (u // 3), side)
        return dz, dy

    def peer_at(dx, core, step):
        dz, dy = away(step)
        return (lax.rem(me_x + dx, side) * 2 + core) * n + lax.rem(me_z + dz, side) * side + lax.rem(me_y + dy, side)

    def signal(step, carry):
        for dx in far:
            for core in range(2):
                peer = peer_at(dx, core, step)

                @pl.when(peer != me)
                def _():
                    pl.semaphore_signal(barrier, inc=1, device_id=device(peer), device_id_type=MESH)
        return carry

    lax.fori_loop(0, n, signal, 0)
    hot_load = pltpu.make_async_copy(hot_hbm, hot, lsems.at[0])
    cold_load = pltpu.make_async_copy(cold_hbm, cold, lsems.at[1])
    w_load = pltpu.make_async_copy(w_hbm, w_ref, lsems.at[2])
    hot_load.start()
    w_load.start()
    cold_load.start()
    for load in small:
        load.wait()
    wanted = req_ref[0].astype(f32)
    wanted = jnp.concatenate([wanted, jnp.zeros((total - wanted.shape[0], total), f32)], axis=0).T
    asks[...] = wanted.reshape(total, 1, total)
    tok = tok_ref[...].astype(f32)
    is_hot = tok < float(hot_count)
    row = lax.broadcasted_iota(jnp.int32, (tokens, tokens), 0)
    earlier = row < lax.broadcasted_iota(jnp.int32, (tokens, tokens), 1)
    marks = jnp.broadcast_to(jnp.where(is_hot, 1.0, 0.0), (8, tokens)).astype(bf)
    before = jnp.dot(marks, jnp.where(earlier, 1.0, 0.0).astype(bf), preferred_element_type=f32)[0:1]
    place = lax.broadcasted_iota(jnp.int32, (1, tokens), 1).astype(f32)
    rank = jnp.where(is_hot, before, half + place - before)
    info[0:1] = seg_ref[...].astype(f32)
    info[1:2] = rank
    rank_t[...] = jnp.broadcast_to(rank, (128, tokens)).T

    def unpacker(ranks, first, count):
        packed_row = lax.broadcasted_iota(jnp.int32, (count, tokens), 0).astype(f32) + float(first)
        return jnp.where(packed_row == ranks, 1.0, 0.0).astype(bf)

    packed[...] = select_exact(unpacker(rank, 0, tokens), jnp.broadcast_to(tok, (128, tokens)).T)
    pl.semaphore_wait(barrier, total - 1)

    def ask(peer, src):
        return pltpu.make_async_remote_copy(
            src_ref=asks.at[peer], dst_ref=asked.at[src], send_sem=msems.at[0], recv_sem=msems.at[1],
            device_id=device(peer), device_id_type=MESH,
        )

    def start_ask(step, carry):
        for dx in far:
            for core in range(2):
                peer = peer_at(dx, core, step)

                @pl.when(peer != me)
                def _():
                    ask(peer, me).start()
        return carry

    lax.fori_loop(0, n, start_ask, 0)

    def tell(step, carry):
        pltpu.make_async_remote_copy(
            src_ref=info, dst_ref=info_ref.at[me_s], send_sem=msems.at[4], recv_sem=msems.at[5],
            device_id={"seq": lax.rem(me_s + step, n)}, device_id_type=MESH,
        ).start()
        return carry

    lax.fori_loop(1, n, tell, 0)
    asked[me] = asks[me]
    info_ref[me_s] = info[...]

    def sweep(ids, table, count):
        gat[...] = jnp.zeros_like(gat)

        def add(step, inner):
            base = step * wide
            pick = one_hot(ids, base.astype(f32), wide)
            block = table[pl.ds(pl.multiple_of(base, wide), wide), :]
            gat[...] += jnp.dot(pick, block, preferred_element_type=f32)
            return inner

        lax.fori_loop(0, count // wide, add, 0)

    def part_copy(part, peer, src):
        span = pl.ds(part * half, half)
        return pltpu.make_async_remote_copy(
            src_ref=send.at[peer, :, span], dst_ref=recv.at[src, :, span], send_sem=msems.at[6 + part],
            recv_sem=msems.at[8] if part == 0 else crecvs.at[src],
            device_id={"seq": peer}, device_id_type=MESH,
        )

    def project(part, x):
        span = slice(part * half, part * half + half)
        for dz in far:
            z = lax.rem(me_z + dz, side)
            block = w_ref[:, pl.ds(pl.multiple_of(z * 512, 512), 512)]
            out = jnp.dot(x, block, preferred_element_type=f32).astype(bf).T
            for y in range(side):
                gates[z * side + y, :, span] = out[y * 128:y * 128 + 32]
                send[z * side + y, :, span] = out[y * 128 + 32:y * 128 + 128]
            for dy in far:
                if (dz, dy) != (0, 0):
                    part_copy(part, z * side + lax.rem(me_y + dy, side), me_s).start()
        recv[me_s, :, span] = send[me_s, :, span]

    hot_load.wait()
    sweep(packed[0:half], hot, hot_count)
    found = gat[...].astype(bf)
    emb_packed[0:half] = found
    w_load.wait()
    project(0, normalize(found))

    def all_of(src, dst, count, a, b, span=None):
        every = pl.ds(0, count)
        src = src.at[every] if span is None else src.at[every, :, span]
        dst = dst.at[every] if span is None else dst.at[every, :, span]
        return pltpu.make_async_remote_copy(
            src_ref=src, dst_ref=dst, send_sem=msems.at[a], recv_sem=msems.at[b],
            device_id=device(me), device_id_type=MESH,
        )

    ask_all = all_of(asks, asked, total - 1, 0, 1)
    row_all = all_of(rows_out, rows_in, total - 1, 2, 3)
    info_all = all_of(info_ref, info_ref, n - 1, 4, 5)
    hot_all = all_of(send, recv, n - 1, 6, 8, pl.ds(0, half))
    cold_all = all_of(send, recv, n - 1, 7, 8, pl.ds(half, half))
    ask_all.wait_recv()
    slot = lax.broadcasted_iota(jnp.int32, (slots, 128), 0)
    lane = lax.broadcasted_iota(jnp.int32, (slots, 128), 1)
    ids = select_exact(jnp.where(slot // 4 == lane, 1.0, 0.0).astype(bf), asked[...].reshape(total, 128))
    ids = jnp.sum(jnp.where(lax.rem(slot, 4) == lane, ids, 0.0), axis=1, keepdims=True)
    idx[...] = jnp.broadcast_to(ids, (slots, 128))
    cold_load.wait()

    def give(peer, src):
        return pltpu.make_async_remote_copy(
            src_ref=rows_out.at[peer], dst_ref=rows_in.at[src], send_sem=msems.at[2], recv_sem=msems.at[3],
            device_id=device(peer), device_id_type=MESH,
        )

    def serve(first, second):
        group = total // side
        spans = [lax.rem(me_x + dx, side) for dx in (first, second)]
        mine = jnp.concatenate(
            [idx[pl.ds(pl.multiple_of(x * group * 4, group * 4), group * 4), :] for x in spans], axis=0
        )
        sweep(mine, cold, cold_count)
        for c, x in enumerate(spans):
            part = gat[c * group * 4:(c + 1) * group * 4, :].astype(bf)
            rows_out[pl.ds(x * group, group)] = part.reshape(group, 4, part.shape[1])

        def start_give(step, inner):
            for dx in (first, second):
                for core in range(2):
                    peer = peer_at(dx, core, step)

                    @pl.when(peer != me)
                    def _():
                        give(peer, me).start()
            return inner

        lax.fori_loop(0, n, start_give, 0)

    serve(2, 1)
    serve(3, 0)
    rows_in[me] = rows_out[me]
    ask_all.wait_send()
    info_all.wait_recv()
    hot_all.wait_recv()

    def unpack_hot(src, carry):
        pick = unpacker(info_ref[src][1:2], 0, half)
        qkv_ref[src] = jnp.dot(recv[src, :, 0:half], pick, preferred_element_type=f32).astype(bf)
        return carry

    lax.fori_loop(0, n, unpack_hot, 0, unroll=2)
    row_all.wait_recv()
    flat[...] = rows_in[...].reshape(flat.shape)
    pick = one_hot(packed[half:tokens], float(hot_count), slots)
    found = jnp.dot(pick, flat[...], preferred_element_type=f32).astype(bf)
    emb_packed[half:tokens] = found
    project(1, normalize(found))
    pick = one_hot(rank_t[...], 0.0, tokens)
    emb_ref[...] = jnp.dot(pick, emb_packed[...], preferred_element_type=f32).astype(bf)
    pick = unpacker(info[1:2], 0, tokens)
    opened = jnp.dot(gates[...].reshape(tokens, tokens), pick, preferred_element_type=f32).astype(bf)
    gate_ref[...] = opened.reshape(gate_ref.shape)

    def unpack_cold(src):
        pick = unpacker(info_ref[src][1:2], half, half)
        more = jnp.dot(recv[src, :, half:tokens], pick, preferred_element_type=f32)
        qkv_ref[src] = (qkv_ref[src].astype(f32) + more).astype(bf)

    unpack_cold(me_s)

    def arrive(step, carry):
        dz, dy = away(step)
        src = lax.rem(me_z + side - dz, side) * side + lax.rem(me_y + side - dy, side)
        part_copy(1, src, src).wait_recv()
        unpack_cold(src)
        return carry

    lax.fori_loop(0, n - 1, arrive, 0)
    row_all.wait_send()
    info_all.wait_send()
    hot_all.wait_send()
    cold_all.wait_send()


def front(token_rows, segment_ids, requests, hot_table, cold_table, weight, n, m):
    tokens = token_rows.shape[1]
    width = hot_table.shape[1]
    total = n * m
    slots = total * requests.shape[1]
    bf = jnp.bfloat16
    f32 = jnp.float32
    vm = pl.BlockSpec(memory_space=pltpu.VMEM)
    hbm = pl.BlockSpec(memory_space=pltpu.HBM)
    operands = (token_rows, segment_ids, requests, hot_table, cold_table, weight)
    return pl.pallas_call(
        functools.partial(front_kernel, n, m),
        out_shape=(
            jax.ShapeDtypeStruct((tokens, width), bf),
            jax.ShapeDtypeStruct((n, 32, tokens), bf),
            jax.ShapeDtypeStruct((n, 96, tokens), bf),
            jax.ShapeDtypeStruct((n, 2, tokens), f32),
        ),
        in_specs=[hbm] * 6,
        out_specs=(vm, vm, vm, vm),
        scratch_shapes=[
            pltpu.VMEM(token_rows.shape, jnp.int32),
            pltpu.VMEM(segment_ids.shape, jnp.int32),
            pltpu.VMEM(requests.shape, jnp.int32),
            pltpu.VMEM(hot_table.shape, bf),
            pltpu.VMEM(cold_table.shape, bf),
            pltpu.VMEM(weight.shape, bf),
            pltpu.VMEM((n, 96, tokens), bf),
            pltpu.VMEM((n, 96, tokens), bf),
            pltpu.VMEM((n, 32, tokens), bf),
            pltpu.VMEM((tokens, width), bf),
            pltpu.VMEM((2, tokens), f32),
            pltpu.VMEM((total, 1, 128), f32),
            pltpu.VMEM((total, 1, 128), f32),
            pltpu.VMEM((total, 4, width), bf),
            pltpu.VMEM((total, 4, width), bf),
            pltpu.VMEM((slots // 2, width), f32),
            pltpu.VMEM((tokens, 128), f32),
            pltpu.VMEM((tokens, 128), f32),
            pltpu.VMEM((slots, 128), f32),
            pltpu.VMEM((slots, width), bf),
            pltpu.SemaphoreType.DMA((9,)),
            pltpu.SemaphoreType.DMA((n,)),
            pltpu.SemaphoreType.DMA((6,)),
        ],
        compiler_params=pltpu.CompilerParams(collective_id=1, has_side_effects=True, vmem_limit_bytes=48 << 20),
        name="front",
    )(*[pltpu.with_memory_space_constraint(x, pltpu.HBM) for x in operands])


def greet(axis_size):
    me = lax.axis_index("seq")
    barrier = pltpu.get_barrier_semaphore()

    def signal(step, carry):
        peer = lax.rem(me + step, axis_size)
        pl.semaphore_signal(barrier, inc=1, device_id={"seq": peer}, device_id_type=MESH)
        return carry

    lax.fori_loop(1, axis_size, signal, 0)
    pl.semaphore_wait(barrier, axis_size - 1)


def finish_kernel(n, att_ref, gate_ref, emb_ref, wo, up, down, out_ref, back, open_gate, sends, recvs):
    me = lax.axis_index("seq")
    greet(n)

    def copy_to(peer, src):
        return pltpu.make_async_remote_copy(
            src_ref=att_ref.at[peer], dst_ref=back.at[src], send_sem=sends.at[peer], recv_sem=recvs.at[src],
            device_id={"seq": peer}, device_id_type=MESH,
        )

    side = 4
    far = (2, 1, 3, 0)
    for dz in far:
        for dy in far:
            if (dz, dy) != (0, 0):
                peer = lax.rem(me // side + dz, side) * side + lax.rem(me + dy, side)
                copy_to(peer, me).start()
    back[me] = att_ref[me]

    def open_one(step, carry):
        gate = gate_ref[step].astype(jnp.float32)
        open_gate[step] = gate / (1.0 + jnp.exp(-gate))
        return carry

    lax.fori_loop(0, n, open_one, 0)

    def finish(step, carry):
        source = lax.rem(me + n - step, n)
        peer = lax.rem(me + step, n)
        copy_to(peer, me).wait_send()
        copy_to(peer, source).wait_recv()
        return carry

    lax.fori_loop(1, n, finish, 0)
    rows = 256

    def tail(step, carry):
        span = pl.ds(pl.multiple_of(step * rows, rows), rows)
        att = back[:, :, span].reshape(n * 32, rows).astype(jnp.float32)
        gate = open_gate[:, :, span].reshape(n * 32, rows)
        scale = lax.rsqrt(jnp.mean(att * att, axis=0, keepdims=True) + epsilon)
        heads = (att * scale * gate).astype(jnp.bfloat16).T
        hidden = emb_ref[span, :].astype(jnp.float32) + jnp.dot(heads, wo[...], preferred_element_type=jnp.float32)
        normed = (hidden * lax.rsqrt(jnp.mean(hidden * hidden, axis=-1, keepdims=True) + epsilon)).astype(jnp.bfloat16)
        wide = jnp.dot(normed, up[...], preferred_element_type=jnp.float32)
        active = (wide / (1.0 + jnp.exp(-wide))).astype(jnp.bfloat16)
        out = hidden + jnp.dot(active, down[...], preferred_element_type=jnp.float32)
        out_ref[span, :] = out.astype(jnp.bfloat16)
        return carry

    lax.fori_loop(0, emb_ref.shape[0] // rows, tail, 0)


def finish_layer(attended, gate, embedded, wo, up, down, n):
    tokens, width = embedded.shape
    bf = jnp.bfloat16
    vm = pl.BlockSpec(memory_space=pltpu.VMEM)
    return pl.pallas_call(
        functools.partial(finish_kernel, n),
        out_shape=jax.ShapeDtypeStruct((tokens, width), bf),
        in_specs=[vm] * 6,
        out_specs=vm,
        scratch_shapes=[
            pltpu.VMEM((n, 32, tokens), bf),
            pltpu.VMEM((n, 32, tokens), jnp.float32),
            pltpu.SemaphoreType.DMA((n,)),
            pltpu.SemaphoreType.DMA((n,)),
        ],
        compiler_params=pltpu.CompilerParams(collective_id=2, has_side_effects=True, vmem_limit_bytes=20 << 20),
        name="finish",
    )(attended, gate, embedded, wo, up, down)


def local(token_rows, segment_ids, requests, hot_table, cold_table, input_weight, output_weight, up_weight, down_weight):
    n = lax.axis_size("seq")
    m = lax.axis_size("emb")
    embedded, gate, triples, segments = front(
        token_rows, segment_ids, jnp.transpose(requests, (0, 2, 1)), hot_table, cold_table, input_weight, n, m
    )
    attended = attention(segments, triples, 4)
    return finish_layer(attended, gate, embedded, output_weight, up_weight, down_weight, n)[None]


def solution(mesh):
    placed = (
        P("emb", "seq"), P("emb", "seq"), P(("emb", "seq"), None, None), P(), P(("emb", "seq"), None), P(), P(), P(), P(),
    )
    return jax.shard_map(local, mesh=mesh, in_specs=placed, out_specs=P("emb", "seq", None), check_vma=False)
```

```python
import functools

import jax
import jax.numpy as jnp
from jax import lax
from jax.experimental import pallas as pl
from jax.experimental.pallas import tpu as pltpu
from jax.sharding import PartitionSpec as P

epsilon = 1e-06

BIG = float(2 ** 30)


def attn_kernel(U, info_ref, q_ref, k_ref, v_ref, out_ref, a_scr, accs):
    blocks, _, W = q_ref.shape
    bf = jnp.bfloat16
    f32 = jnp.float32
    half = W // 2
    segments = info_ref[:, 0:1, :]
    s1, s2, s3 = [jnp.sum((segments < s).astype(f32)).astype(jnp.int32) for s in (1, 2, 3)]
    causal = lax.broadcasted_iota(jnp.int32, (half, half), 0) <= lax.broadcasted_iota(jnp.int32, (half, half), 1)

    def silu(s):
        h = s.astype(bf)
        return h + h * jnp.tanh(h)

    def keys(first, count):
        return k_ref[pl.ds(pl.multiple_of(first, count), count), :]

    def weigh_own(slot, i):
        q = q_ref[i]
        early = silu(jnp.dot(keys(i * W, half), q, preferred_element_type=f32))
        late = silu(jnp.dot(keys(i * W + half, half), q[:, half:], preferred_element_type=f32))
        zero = jnp.zeros((half, half), bf)
        a_scr[slot, 0:half, 0:half] = jnp.where(causal, early[:, 0:half], zero)
        a_scr[slot, 0:half, half:W] = early[:, half:]
        a_scr[slot, half:W, half:W] = jnp.where(causal, late, zero)

    def gather_own(slot, i):
        v = v_ref[i]
        accs[i, :, 0:half] = jnp.dot(v[:, 0:half], a_scr[slot, 0:half, 0:half], preferred_element_type=f32)
        accs[i, :, half:W] = jnp.dot(v, a_scr[slot, :, half:W], preferred_element_type=f32)

    def low(i):
        first = i * W
        start = jnp.where(first >= s3, s3, jnp.where(first >= s2, s2, jnp.where(first >= s1, s1, 0)))
        return jnp.minimum(start // W, i - 1)

    total = lax.fori_loop(1, blocks, lambda i, c: c + (i - low(i)), 0)

    def after(i, j):
        last = j <= low(i)
        return jnp.where(last, i + 1, i), jnp.where(last, i, j - 1)

    def weigh(slot, i, j, valid):
        i = jnp.where(valid, i, 0)
        j = jnp.where(valid, j, 0)
        a_scr[slot] = silu(jnp.dot(keys(j * W, W), q_ref[i], preferred_element_type=f32))

    def gather(slot, i, j, valid):
        i = jnp.where(valid, i, blocks)
        j = jnp.where(valid, j, 0)
        accs[i] = accs[i] + jnp.dot(v_ref[j], a_scr[slot], preferred_element_type=f32)

    def some(n, i, j):
        out = []
        for u in range(U):
            out.append((i, j, n * U + u < total))
            i, j = after(i, j)
        return out, i, j

    accs[blocks] = jnp.zeros(accs.shape[1:], f32)
    for u in range(U):
        weigh_own(u, u)

    def own_body(g, carry):
        for u in range(U):
            gather_own(u, g * U + u)
            weigh_own(u, (g + 1) * U + u)
        return carry

    lax.fori_loop(0, blocks // U - 1, own_body, 0)
    one, zero = jnp.int32(1), jnp.int32(0)
    head, i1, j1 = some(0, one, zero)
    for u in range(U):
        gather_own(u, blocks - U + u)
        weigh(u, *head[u])

    def body(n, carry):
        i, j, ni, nj = carry
        now, _, _ = some(n, i, j)
        then, mi, mj = some(n + 1, ni, nj)
        for u in range(U):
            gather(u, *now[u])
            weigh(u, *then[u])
        return ni, nj, mi, mj

    lax.fori_loop(0, (total + U - 1) // U, body, (one, zero, i1, j1))
    for i in range(blocks):
        out_ref[i] = accs[i].astype(bf)


def attention(info, q, k, v, U):
    blocks, _, W = q.shape
    bf = jnp.bfloat16
    vm = pl.BlockSpec(memory_space=pltpu.VMEM)
    return pl.pallas_call(
        functools.partial(attn_kernel, U),
        out_shape=jax.ShapeDtypeStruct((blocks, 32, W), bf),
        in_specs=[vm] * 4,
        out_specs=vm,
        scratch_shapes=[pltpu.VMEM((U, W, W), bf), pltpu.VMEM((blocks + 1, 32, W), jnp.float32)],
        compiler_params=pltpu.CompilerParams(vmem_limit_bytes=16 << 20),
        name="attn",
    )(info, q, k, v)


MESH = pl.DeviceIdType.MESH


def one_hot(ids, base, width):
    lane = lax.broadcasted_iota(jnp.int32, ids.shape, 1).astype(jnp.float32)
    pieces = [
        jnp.where(ids == lane + (base + 128 * c), 1.0, 0.0).astype(jnp.bfloat16) for c in range(width // 128)
    ]
    return jnp.concatenate(pieces, axis=1)


def normalize(values):
    x = values.astype(jnp.float32)
    return (x * lax.rsqrt(jnp.mean(x * x, axis=-1, keepdims=True) + epsilon)).astype(jnp.bfloat16)


def select_exact(pick, ids):
    high = jnp.floor(ids * (1.0 / 64.0))
    low = ids - high * 64.0
    return 64.0 * jnp.dot(pick, high.astype(jnp.bfloat16), preferred_element_type=jnp.float32) + jnp.dot(
        pick, low.astype(jnp.bfloat16), preferred_element_type=jnp.float32
    )


def front_kernel(
    n, m, tok_hbm, seg_hbm, req_hbm, hot_hbm, cold_hbm, w_hbm, emb_ref, gate_ref, q_ref, k_ref, v_ref, info_ref,
    part, tok_ref, seg_ref, req_ref, hot, cold, w_ref, send, recv, gates, emb_packed, info, asks, asked,
    rows_out, rows_in, gat, packed, rank_t, idx, flat, msems, crecvs, lsems,
):
    side = 4
    me_s = lax.axis_index("seq")
    me = lax.axis_index("emb") * n + me_s
    me_z, me_y = me_s // side, lax.rem(me_s, side)
    me_x = lax.axis_index("emb") // 2
    total = n * m
    bf = jnp.bfloat16
    f32 = jnp.float32
    hot_count = hot_hbm.shape[0]
    cold_count = cold_hbm.shape[0]
    tokens = tok_hbm.shape[1]
    half = tokens // 2
    slots = idx.shape[0]
    far = (2, 1, 3, 0)
    wide = 2048
    scale = 0.5 / (32.0 ** 0.5)

    barrier = pltpu.get_barrier_semaphore()
    small = [
        pltpu.make_async_copy(a, b, lsems.at[3 + c])
        for c, (a, b) in enumerate(((tok_hbm, tok_ref), (req_hbm, req_ref), (seg_hbm, seg_ref)))
    ]
    for load in small:
        load.start()

    def device(peer):
        return {"emb": peer // n, "seq": lax.rem(peer, n)}

    def away(step):
        t = step // side
        u = lax.rem(step, side)
        dz = lax.rem(2 + 3 * t + 3 * (t // 2) + 2 * (t // 3), side)
        dy = lax.rem(2 + 3 * u + 3 * (u // 2) + 2 * (u // 3), side)
        return dz, dy

    def peer_at(dx, core, step):
        dz, dy = away(step)
        return (lax.rem(me_x + dx, side) * 2 + core) * n + lax.rem(me_z + dz, side) * side + lax.rem(me_y + dy, side)

    def signal(step, carry):
        for dx in far:
            for core in range(2):
                peer = peer_at(dx, core, step)

                @pl.when(peer != me)
                def _():
                    pl.semaphore_signal(barrier, inc=1, device_id=device(peer), device_id_type=MESH)
        return carry

    lax.fori_loop(0, n, signal, 0)
    hot_load = pltpu.make_async_copy(hot_hbm, hot, lsems.at[0])
    cold_load = pltpu.make_async_copy(cold_hbm, cold, lsems.at[1])
    w_load = pltpu.make_async_copy(w_hbm, w_ref, lsems.at[2])
    hot_load.start()
    w_load.start()
    cold_load.start()
    for load in small:
        load.wait()
    wanted = req_ref[0].astype(f32)
    wanted = jnp.concatenate([wanted, jnp.zeros((total - wanted.shape[0], total), f32)], axis=0).T
    asks[...] = wanted.reshape(total, 1, total)
    tok = tok_ref[...].astype(f32)
    is_hot = tok < float(hot_count)
    row = lax.broadcasted_iota(jnp.int32, (tokens, tokens), 0)
    earlier = row < lax.broadcasted_iota(jnp.int32, (tokens, tokens), 1)
    marks = jnp.broadcast_to(jnp.where(is_hot, 1.0, 0.0), (8, tokens)).astype(bf)
    before = jnp.dot(marks, jnp.where(earlier, 1.0, 0.0).astype(bf), preferred_element_type=f32)[0:1]
    place = lax.broadcasted_iota(jnp.int32, (1, tokens), 1).astype(f32)
    rank = jnp.where(is_hot, before, half + place - before)
    info[0:1] = seg_ref[...].astype(f32)
    info[1:2] = rank
    rank_t[...] = jnp.broadcast_to(rank, (128, tokens)).T

    def unpacker(ranks, first, count):
        packed_row = lax.broadcasted_iota(jnp.int32, (count, tokens), 0).astype(f32) + float(first)
        return jnp.where(packed_row == ranks, 1.0, 0.0).astype(bf)

    packed[...] = select_exact(unpacker(rank, 0, tokens), jnp.broadcast_to(tok, (128, tokens)).T)
    pl.semaphore_wait(barrier, total - 1)

    def ask(peer, src):
        return pltpu.make_async_remote_copy(
            src_ref=asks.at[peer], dst_ref=asked.at[src], send_sem=msems.at[0], recv_sem=msems.at[1],
            device_id=device(peer), device_id_type=MESH,
        )

    def start_ask(step, carry):
        for dx in far:
            for core in range(2):
                peer = peer_at(dx, core, step)

                @pl.when(peer != me)
                def _():
                    ask(peer, me).start()
        return carry

    lax.fori_loop(0, n, start_ask, 0)

    def tell(step, carry):
        pltpu.make_async_remote_copy(
            src_ref=info, dst_ref=info_ref.at[me_s], send_sem=msems.at[4], recv_sem=msems.at[5],
            device_id={"seq": lax.rem(me_s + step, n)}, device_id_type=MESH,
        ).start()
        return carry

    lax.fori_loop(1, n, tell, 0)
    asked[me] = asks[me]
    info_ref[me_s] = info[...]

    def sweep(ids, table, count):
        gat[...] = jnp.zeros_like(gat)

        def add(step, inner):
            base = step * wide
            pick = one_hot(ids, base.astype(f32), wide)
            block = table[pl.ds(pl.multiple_of(base, wide), wide), :]
            gat[...] += jnp.dot(pick, block, preferred_element_type=f32)
            return inner

        lax.fori_loop(0, count // wide, add, 0)

    def part_copy(piece, peer, src):
        span = pl.ds(piece * half, half)
        return pltpu.make_async_remote_copy(
            src_ref=send.at[peer, :, span], dst_ref=recv.at[src, :, span], send_sem=msems.at[6 + piece],
            recv_sem=msems.at[8] if piece == 0 else crecvs.at[src],
            device_id={"seq": peer}, device_id_type=MESH,
        )

    def project(piece, x):
        span = slice(piece * half, piece * half + half)
        for dz in far:
            z = lax.rem(me_z + dz, side)
            block = w_ref[:, pl.ds(pl.multiple_of(z * 512, 512), 512)]
            out = jnp.dot(x, block, preferred_element_type=f32).astype(bf).T
            for y in range(side):
                gates[z * side + y, :, span] = out[y * 128:y * 128 + 32]
                send[z * side + y, :, span] = out[y * 128 + 32:y * 128 + 128]
            for dy in far:
                if (dz, dy) != (0, 0):
                    part_copy(piece, z * side + lax.rem(me_y + dy, side), me_s).start()
        recv[me_s, :, span] = send[me_s, :, span]

    hot_load.wait()
    sweep(packed[0:half], hot, hot_count)
    found = gat[...].astype(bf)
    emb_packed[0:half] = found
    w_load.wait()
    project(0, normalize(found))

    def all_of(src, dst, count, a, b, span=None):
        every = pl.ds(0, count)
        src = src.at[every] if span is None else src.at[every, :, span]
        dst = dst.at[every] if span is None else dst.at[every, :, span]
        return pltpu.make_async_remote_copy(
            src_ref=src, dst_ref=dst, send_sem=msems.at[a], recv_sem=msems.at[b],
            device_id=device(me), device_id_type=MESH,
        )

    ask_all = all_of(asks, asked, total - 1, 0, 1)
    row_all = all_of(rows_out, rows_in, total - 1, 2, 3)
    info_all = all_of(info_ref, info_ref, n - 1, 4, 5)
    hot_all = all_of(send, recv, n - 1, 6, 8, pl.ds(0, half))
    cold_all = all_of(send, recv, n - 1, 7, 8, pl.ds(half, half))
    ask_all.wait_recv()
    slot = lax.broadcasted_iota(jnp.int32, (slots, 128), 0)
    lane = lax.broadcasted_iota(jnp.int32, (slots, 128), 1)
    ids = select_exact(jnp.where(slot // 4 == lane, 1.0, 0.0).astype(bf), asked[...].reshape(total, 128))
    ids = jnp.sum(jnp.where(lax.rem(slot, 4) == lane, ids, 0.0), axis=1, keepdims=True)
    idx[...] = jnp.broadcast_to(ids, (slots, 128))
    cold_load.wait()

    def give(peer, src):
        return pltpu.make_async_remote_copy(
            src_ref=rows_out.at[peer], dst_ref=rows_in.at[src], send_sem=msems.at[2], recv_sem=msems.at[3],
            device_id=device(peer), device_id_type=MESH,
        )

    def serve(first, second):
        group = total // side
        spans = [lax.rem(me_x + dx, side) for dx in (first, second)]
        mine = jnp.concatenate(
            [idx[pl.ds(pl.multiple_of(x * group * 4, group * 4), group * 4), :] for x in spans], axis=0
        )
        sweep(mine, cold, cold_count)
        for c, x in enumerate(spans):
            share = gat[c * group * 4:(c + 1) * group * 4, :].astype(bf)
            rows_out[pl.ds(x * group, group)] = share.reshape(group, 4, share.shape[1])

        def start_give(step, inner):
            for dx in (first, second):
                for core in range(2):
                    peer = peer_at(dx, core, step)

                    @pl.when(peer != me)
                    def _():
                        give(peer, me).start()
            return inner

        lax.fori_loop(0, n, start_give, 0)

    serve(2, 1)
    serve(3, 0)
    rows_in[me] = rows_out[me]
    ask_all.wait_send()
    info_all.wait_recv()
    hot_all.wait_recv()

    def unpack_hot(src, carry):
        pick = unpacker(info_ref[src][1:2], 0, half)
        part[src] = jnp.dot(recv[src, :, 0:half], pick, preferred_element_type=f32).astype(bf)
        return carry

    lax.fori_loop(0, n, unpack_hot, 0, unroll=2)
    row_all.wait_recv()
    flat[...] = rows_in[...].reshape(flat.shape)
    pick = one_hot(packed[half:tokens], float(hot_count), slots)
    found = jnp.dot(pick, flat[...], preferred_element_type=f32).astype(bf)
    emb_packed[half:tokens] = found
    project(1, normalize(found))
    pick = one_hot(rank_t[...], 0.0, tokens)
    emb_ref[...] = jnp.dot(pick, emb_packed[...], preferred_element_type=f32).astype(bf)
    pick = unpacker(info[1:2], 0, tokens)
    opened = jnp.dot(gates[...].reshape(tokens, tokens), pick, preferred_element_type=f32).astype(bf)
    gate_ref[...] = opened.reshape(gate_ref.shape)

    def unpack_cold(src):
        pick = unpacker(info_ref[src][1:2], half, half)
        more = jnp.dot(recv[src, :, half:tokens], pick, preferred_element_type=f32)
        whole = part[src].astype(f32) + more
        v_ref[src] = whole[0:32].astype(bf)
        q_ref[src, 0:32] = (whole[32:64] * scale).astype(bf)
        row = lax.broadcasted_iota(jnp.int32, (16, tokens), 0).astype(f32)
        same = jnp.where(info_ref[src][0:1] == row, 1.0, 0.0)
        q_ref[src, 32:48] = same.astype(bf)
        bias = jnp.where(row < 4.0, (1.0 - same) * (-BIG), 0.0)
        extended = jnp.concatenate([whole[64:96], bias], axis=0).astype(bf)
        k_ref[pl.ds(pl.multiple_of(src * tokens, tokens), tokens), :] = extended.T

    unpack_cold(me_s)

    def arrive(step, carry):
        dz, dy = away(step)
        src = lax.rem(me_z + side - dz, side) * side + lax.rem(me_y + side - dy, side)
        part_copy(1, src, src).wait_recv()
        unpack_cold(src)
        return carry

    lax.fori_loop(0, n - 1, arrive, 0)
    row_all.wait_send()
    info_all.wait_send()
    hot_all.wait_send()
    cold_all.wait_send()


def front(token_rows, segment_ids, requests, hot_table, cold_table, weight, n, m):
    tokens = token_rows.shape[1]
    width = hot_table.shape[1]
    total = n * m
    slots = total * requests.shape[1]
    bf = jnp.bfloat16
    f32 = jnp.float32
    vm = pl.BlockSpec(memory_space=pltpu.VMEM)
    hbm = pl.BlockSpec(memory_space=pltpu.HBM)
    operands = (token_rows, segment_ids, requests, hot_table, cold_table, weight)
    return pl.pallas_call(
        functools.partial(front_kernel, n, m),
        out_shape=(
            jax.ShapeDtypeStruct((tokens, width), bf),
            jax.ShapeDtypeStruct((n, 32, tokens), bf),
            jax.ShapeDtypeStruct((n, 48, tokens), bf),
            jax.ShapeDtypeStruct((n * tokens, 48), bf),
            jax.ShapeDtypeStruct((n, 32, tokens), bf),
            jax.ShapeDtypeStruct((n, 2, tokens), f32),
        ),
        in_specs=[hbm] * 6,
        out_specs=(vm,) * 6,
        scratch_shapes=[
            pltpu.VMEM((n, 96, tokens), bf),
            pltpu.VMEM(token_rows.shape, jnp.int32),
            pltpu.VMEM(segment_ids.shape, jnp.int32),
            pltpu.VMEM(requests.shape, jnp.int32),
            pltpu.VMEM(hot_table.shape, bf),
            pltpu.VMEM(cold_table.shape, bf),
            pltpu.VMEM(weight.shape, bf),
            pltpu.VMEM((n, 96, tokens), bf),
            pltpu.VMEM((n, 96, tokens), bf),
            pltpu.VMEM((n, 32, tokens), bf),
            pltpu.VMEM((tokens, width), bf),
            pltpu.VMEM((2, tokens), f32),
            pltpu.VMEM((total, 1, 128), f32),
            pltpu.VMEM((total, 1, 128), f32),
            pltpu.VMEM((total, 4, width), bf),
            pltpu.VMEM((total, 4, width), bf),
            pltpu.VMEM((slots // 2, width), f32),
            pltpu.VMEM((tokens, 128), f32),
            pltpu.VMEM((tokens, 128), f32),
            pltpu.VMEM((slots, 128), f32),
            pltpu.VMEM((slots, width), bf),
            pltpu.SemaphoreType.DMA((9,)),
            pltpu.SemaphoreType.DMA((n,)),
            pltpu.SemaphoreType.DMA((6,)),
        ],
        compiler_params=pltpu.CompilerParams(collective_id=1, has_side_effects=True, vmem_limit_bytes=46 << 20),
        name="front",
    )(*[pltpu.with_memory_space_constraint(x, pltpu.HBM) for x in operands])


def greet(axis_size):
    me = lax.axis_index("seq")
    barrier = pltpu.get_barrier_semaphore()

    def signal(step, carry):
        peer = lax.rem(me + step, axis_size)
        pl.semaphore_signal(barrier, inc=1, device_id={"seq": peer}, device_id_type=MESH)
        return carry

    lax.fori_loop(1, axis_size, signal, 0)
    pl.semaphore_wait(barrier, axis_size - 1)


def finish_kernel(n, att_ref, gate_ref, emb_ref, wo, up, down, out_ref, back, open_gate, sends, recvs):
    me = lax.axis_index("seq")
    greet(n)

    tokens = emb_ref.shape[0]
    rows = tokens // 2

    def copy_to(part, peer):
        return pltpu.make_async_remote_copy(
            src_ref=att_ref.at[peer, :, pl.ds(part * rows, rows)], dst_ref=back.at[part, me], send_sem=sends,
            recv_sem=recvs.at[part], device_id={"seq": peer}, device_id_type=MESH,
        )

    side = 4
    far = (2, 1, 3, 0)
    for part in range(2):
        for dz in far:
            for dy in far:
                if (dz, dy) != (0, 0):
                    copy_to(part, lax.rem(me // side + dz, side) * side + lax.rem(me + dy, side)).start()
    for part in range(2):
        back[part, me] = att_ref[me, :, part * rows:(part + 1) * rows]

    def open_one(step, carry):
        gate = gate_ref[step].astype(jnp.float32)
        open_gate[step] = gate / (1.0 + jnp.exp(-gate))
        return carry

    lax.fori_loop(0, n, open_one, 0)

    every = pl.ds(0, n - 1)

    def tail(step):
        span = slice(step * rows, (step + 1) * rows)
        pltpu.make_async_remote_copy(
            src_ref=back.at[step, every], dst_ref=back.at[step, every], send_sem=sends, recv_sem=recvs.at[step],
            device_id={"seq": me}, device_id_type=MESH,
        ).wait_recv()
        att = back[step].reshape(n * 32, rows).astype(jnp.float32)
        gate = open_gate[:, :, span].reshape(n * 32, rows)
        scale = lax.rsqrt(jnp.mean(att * att, axis=0, keepdims=True) + epsilon)
        heads = (att * scale * gate).astype(jnp.bfloat16).T
        hidden = emb_ref[span, :].astype(jnp.float32) + jnp.dot(heads, wo[...], preferred_element_type=jnp.float32)
        normed = (hidden * lax.rsqrt(jnp.mean(hidden * hidden, axis=-1, keepdims=True) + epsilon)).astype(jnp.bfloat16)
        wide = jnp.dot(normed, up[...], preferred_element_type=jnp.float32)
        active = (wide / (1.0 + jnp.exp(-wide))).astype(jnp.bfloat16)
        out = hidden + jnp.dot(active, down[...], preferred_element_type=jnp.float32)
        out_ref[span, :] = out.astype(jnp.bfloat16)

    for step in range(2):
        tail(step)
    pltpu.make_async_remote_copy(
        src_ref=att_ref.at[every], dst_ref=att_ref.at[every], send_sem=sends, recv_sem=recvs.at[0],
        device_id={"seq": me}, device_id_type=MESH,
    ).wait_send()


def finish_layer(attended, gate, embedded, wo, up, down, n):
    tokens, width = embedded.shape
    bf = jnp.bfloat16
    vm = pl.BlockSpec(memory_space=pltpu.VMEM)
    return pl.pallas_call(
        functools.partial(finish_kernel, n),
        out_shape=jax.ShapeDtypeStruct((tokens, width), bf),
        in_specs=[vm] * 6,
        out_specs=vm,
        scratch_shapes=[
            pltpu.VMEM((2, n, 32, tokens // 2), bf),
            pltpu.VMEM((n, 32, tokens), jnp.float32),
            pltpu.SemaphoreType.DMA,
            pltpu.SemaphoreType.DMA((2,)),
        ],
        compiler_params=pltpu.CompilerParams(collective_id=2, has_side_effects=True, vmem_limit_bytes=20 << 20),
        name="finish",
    )(attended, gate, embedded, wo, up, down)


def local(token_rows, segment_ids, requests, hot_table, cold_table, input_weight, output_weight, up_weight, down_weight):
    n = lax.axis_size("seq")
    m = lax.axis_size("emb")
    embedded, gate, q, k, v, info = front(
        token_rows, segment_ids, jnp.transpose(requests, (0, 2, 1)), hot_table, cold_table, input_weight, n, m
    )
    attended = attention(info, q, k, v, 8)
    return finish_layer(attended, gate, embedded, output_weight, up_weight, down_weight, n)[None]


def solution(mesh):
    placed = (
        P("emb", "seq"), P("emb", "seq"), P(("emb", "seq"), None, None), P(), P(("emb", "seq"), None), P(), P(), P(), P(),
    )
    return jax.shard_map(local, mesh=mesh, in_specs=placed, out_specs=P("emb", "seq", None), check_vma=False)
```

```python
import functools

import jax
import jax.numpy as jnp
from jax import lax
from jax.experimental import pallas as pl
from jax.experimental.pallas import tpu as pltpu
from jax.sharding import PartitionSpec as P

epsilon = 1e-06

BIG = float(2 ** 30)


def silu_half(s):
    h = s.astype(jnp.bfloat16)
    return h + h * jnp.tanh(h)


def attn_kernel(U, info_ref, q_ref, k_ref, v_ref, own_ref, out_ref, a_scr, accs):
    blocks, _, W = q_ref.shape
    bf = jnp.bfloat16
    f32 = jnp.float32
    half = W // 2
    segments = info_ref[:, 0:1, :]
    s1, s2, s3 = [jnp.sum((segments < s).astype(f32)).astype(jnp.int32) for s in (1, 2, 3)]
    for i in range(blocks):
        accs[i] = own_ref[i]
    accs[blocks] = jnp.zeros(accs.shape[1:], f32)

    def low(i):
        first = i * W
        start = jnp.where(first >= s3, s3, jnp.where(first >= s2, s2, jnp.where(first >= s1, s1, 0)))
        return jnp.minimum(start // half, 2 * i - 1)

    total = lax.fori_loop(1, blocks, lambda i, c: c + (2 * i - low(i)), 0)

    def after(i, j):
        last = j <= low(i)
        return jnp.where(last, i + 1, i), jnp.where(last, 2 * i + 1, j - 1)

    def weigh(slot, i, j, valid):
        i = jnp.where(valid, i, 0)
        j = jnp.where(valid, j, 0)
        keys = k_ref[pl.ds(pl.multiple_of(j * half, half), half), :]
        a_scr[slot] = silu_half(jnp.dot(keys, q_ref[i], preferred_element_type=f32))

    def gather(slot, i, j, valid):
        i = jnp.where(valid, i, blocks)
        j = jnp.where(valid, j, 0)
        values = v_ref[j // 2, :, pl.ds(pl.multiple_of(lax.rem(j, 2) * half, half), half)]
        accs[i] = accs[i] + jnp.dot(values, a_scr[slot], preferred_element_type=f32)

    def some(n, i, j):
        out = []
        for u in range(U):
            out.append((i, j, n * U + u < total))
            i, j = after(i, j)
        return out, i, j

    one = jnp.int32(1)
    head, i1, j1 = some(0, one, one)
    for u in range(U):
        weigh(u, *head[u])

    def body(n, carry):
        i, j, ni, nj = carry
        now, _, _ = some(n, i, j)
        then, mi, mj = some(n + 1, ni, nj)
        for u in range(U):
            gather(u, *now[u])
            weigh(u, *then[u])
        return ni, nj, mi, mj

    lax.fori_loop(0, (total + U - 1) // U, body, (one, one, i1, j1))
    for i in range(blocks):
        out_ref[i] = accs[i].astype(bf)


def attention(info, q, k, v, own, U):
    blocks, _, W = q.shape
    bf = jnp.bfloat16
    vm = pl.BlockSpec(memory_space=pltpu.VMEM)
    return pl.pallas_call(
        functools.partial(attn_kernel, U),
        out_shape=jax.ShapeDtypeStruct((blocks, 32, W), bf),
        in_specs=[vm] * 5,
        out_specs=vm,
        scratch_shapes=[pltpu.VMEM((U, W // 2, W), bf), pltpu.VMEM((blocks + 1, 32, W), jnp.float32)],
        compiler_params=pltpu.CompilerParams(vmem_limit_bytes=18 << 20),
        name="attn",
    )(info, q, k, v, own)


MESH = pl.DeviceIdType.MESH


def one_hot(ids, base, width):
    lane = lax.broadcasted_iota(jnp.int32, ids.shape, 1).astype(jnp.float32)
    pieces = [
        jnp.where(ids == lane + (base + 128 * c), 1.0, 0.0).astype(jnp.bfloat16) for c in range(width // 128)
    ]
    return jnp.concatenate(pieces, axis=1)


def normalize(values):
    x = values.astype(jnp.float32)
    return (x * lax.rsqrt(jnp.mean(x * x, axis=-1, keepdims=True) + epsilon)).astype(jnp.bfloat16)


def select_exact(pick, ids):
    high = jnp.floor(ids * (1.0 / 64.0))
    low = ids - high * 64.0
    return 64.0 * jnp.dot(pick, high.astype(jnp.bfloat16), preferred_element_type=jnp.float32) + jnp.dot(
        pick, low.astype(jnp.bfloat16), preferred_element_type=jnp.float32
    )


def front_kernel(
    n, m, tok_hbm, seg_hbm, req_hbm, hot_hbm, cold_hbm, w_hbm, emb_ref, gate_ref, q_ref, k_ref, v_ref, info_ref, own_ref,
    weights, part, tok_ref, seg_ref, req_ref, hot, cold, w_ref, send, recv, gates, emb_packed, info, asks, asked,
    rows_out, rows_in, gat, packed, rank_t, idx, flat, msems, crecvs, lsems,
):
    side = 4
    me_s = lax.axis_index("seq")
    me = lax.axis_index("emb") * n + me_s
    me_z, me_y = me_s // side, lax.rem(me_s, side)
    me_x = lax.axis_index("emb") // 2
    total = n * m
    bf = jnp.bfloat16
    f32 = jnp.float32
    hot_count = hot_hbm.shape[0]
    cold_count = cold_hbm.shape[0]
    tokens = tok_hbm.shape[1]
    half = tokens // 2
    slots = idx.shape[0]
    far = (2, 1, 3, 0)
    wide = 4096
    scale = 0.5 / (32.0 ** 0.5)

    barrier = pltpu.get_barrier_semaphore()
    small = [
        pltpu.make_async_copy(a, b, lsems.at[3 + c])
        for c, (a, b) in enumerate(((tok_hbm, tok_ref), (req_hbm, req_ref), (seg_hbm, seg_ref)))
    ]
    for load in small:
        load.start()

    def device(peer):
        return {"emb": peer // n, "seq": lax.rem(peer, n)}

    def away(step):
        t = step // side
        u = lax.rem(step, side)
        dz = lax.rem(2 + 3 * t + 3 * (t // 2) + 2 * (t // 3), side)
        dy = lax.rem(2 + 3 * u + 3 * (u // 2) + 2 * (u // 3), side)
        return dz, dy

    def peer_at(dx, core, step):
        dz, dy = away(step)
        return (lax.rem(me_x + dx, side) * 2 + core) * n + lax.rem(me_z + dz, side) * side + lax.rem(me_y + dy, side)

    def signal(step, carry):
        for dx in far:
            for core in range(2):
                peer = peer_at(dx, core, step)

                @pl.when(peer != me)
                def _():
                    pl.semaphore_signal(barrier, inc=1, device_id=device(peer), device_id_type=MESH)
        return carry

    lax.fori_loop(0, n, signal, 0)
    hot_load = pltpu.make_async_copy(hot_hbm, hot, lsems.at[0])
    cold_load = pltpu.make_async_copy(cold_hbm, cold, lsems.at[1])
    w_load = pltpu.make_async_copy(w_hbm, w_ref, lsems.at[2])
    hot_load.start()
    w_load.start()
    cold_load.start()
    for load in small:
        load.wait()
    wanted = req_ref[0].astype(f32)
    wanted = jnp.concatenate([wanted, jnp.zeros((total - wanted.shape[0], total), f32)], axis=0).T
    asks[...] = wanted.reshape(total, 1, total)
    tok = tok_ref[...].astype(f32)
    is_hot = tok < float(hot_count)
    row = lax.broadcasted_iota(jnp.int32, (tokens, tokens), 0)
    earlier = row < lax.broadcasted_iota(jnp.int32, (tokens, tokens), 1)
    marks = jnp.broadcast_to(jnp.where(is_hot, 1.0, 0.0), (8, tokens)).astype(bf)
    before = jnp.dot(marks, jnp.where(earlier, 1.0, 0.0).astype(bf), preferred_element_type=f32)[0:1]
    place = lax.broadcasted_iota(jnp.int32, (1, tokens), 1).astype(f32)
    rank = jnp.where(is_hot, before, half + place - before)
    info[0:1] = seg_ref[...].astype(f32)
    info[1:2] = rank
    rank_t[...] = jnp.broadcast_to(rank, (128, tokens)).T

    def unpacker(ranks, first, count):
        packed_row = lax.broadcasted_iota(jnp.int32, (count, tokens), 0).astype(f32) + float(first)
        return jnp.where(packed_row == ranks, 1.0, 0.0).astype(bf)

    packed[...] = select_exact(unpacker(rank, 0, tokens), jnp.broadcast_to(tok, (128, tokens)).T)
    pl.semaphore_wait(barrier, total - 1)

    def ask(peer, src):
        return pltpu.make_async_remote_copy(
            src_ref=asks.at[peer], dst_ref=asked.at[src], send_sem=msems.at[0], recv_sem=msems.at[1],
            device_id=device(peer), device_id_type=MESH,
        )

    def start_ask(step, carry):
        for dx in far:
            for core in range(2):
                peer = peer_at(dx, core, step)

                @pl.when(peer != me)
                def _():
                    ask(peer, me).start()
        return carry

    lax.fori_loop(0, n, start_ask, 0)

    def tell(step, carry):
        pltpu.make_async_remote_copy(
            src_ref=info, dst_ref=info_ref.at[me_s], send_sem=msems.at[4], recv_sem=msems.at[5],
            device_id={"seq": lax.rem(me_s + step, n)}, device_id_type=MESH,
        ).start()
        return carry

    lax.fori_loop(1, n, tell, 0)
    asked[me] = asks[me]
    info_ref[me_s] = info[...]

    def sweep(ids, table, count):
        gat[...] = jnp.zeros_like(gat)

        def add(step, inner):
            base = step * wide
            pick = one_hot(ids, base.astype(f32), wide)
            block = table[pl.ds(pl.multiple_of(base, wide), wide), :]
            gat[...] += jnp.dot(pick, block, preferred_element_type=f32)
            return inner

        lax.fori_loop(0, count // wide, add, 0)

    def part_copy(piece, peer, src):
        span = pl.ds(piece * half, half)
        return pltpu.make_async_remote_copy(
            src_ref=send.at[peer, :, span], dst_ref=recv.at[src, :, span], send_sem=msems.at[6 + piece],
            recv_sem=msems.at[8] if piece == 0 else crecvs.at[src],
            device_id={"seq": peer}, device_id_type=MESH,
        )

    def project(piece, x):
        span = slice(piece * half, piece * half + half)
        for dz in far:
            z = lax.rem(me_z + dz, side)
            block = w_ref[:, pl.ds(pl.multiple_of(z * 512, 512), 512)]
            out = jnp.dot(x, block, preferred_element_type=f32).astype(bf).T
            for y in range(side):
                gates[z * side + y, :, span] = out[y * 128:y * 128 + 32]
                send[z * side + y, :, span] = out[y * 128 + 32:y * 128 + 128]
            for dy in far:
                if (dz, dy) != (0, 0):
                    part_copy(piece, z * side + lax.rem(me_y + dy, side), me_s).start()
        recv[me_s, :, span] = send[me_s, :, span]

    hot_load.wait()
    sweep(packed[0:half], hot, hot_count)
    found = gat[...].astype(bf)
    emb_packed[0:half] = found
    w_load.wait()
    project(0, normalize(found))

    def all_of(src, dst, count, a, b, span=None):
        every = pl.ds(0, count)
        src = src.at[every] if span is None else src.at[every, :, span]
        dst = dst.at[every] if span is None else dst.at[every, :, span]
        return pltpu.make_async_remote_copy(
            src_ref=src, dst_ref=dst, send_sem=msems.at[a], recv_sem=msems.at[b],
            device_id=device(me), device_id_type=MESH,
        )

    ask_all = all_of(asks, asked, total - 1, 0, 1)
    row_all = all_of(rows_out, rows_in, total - 1, 2, 3)
    info_all = all_of(info_ref, info_ref, n - 1, 4, 5)
    hot_all = all_of(send, recv, n - 1, 6, 8, pl.ds(0, half))
    cold_all = all_of(send, recv, n - 1, 7, 8, pl.ds(half, half))
    ask_all.wait_recv()
    slot = lax.broadcasted_iota(jnp.int32, (slots, 128), 0)
    lane = lax.broadcasted_iota(jnp.int32, (slots, 128), 1)
    ids = select_exact(jnp.where(slot // 4 == lane, 1.0, 0.0).astype(bf), asked[...].reshape(total, 128))
    ids = jnp.sum(jnp.where(lax.rem(slot, 4) == lane, ids, 0.0), axis=1, keepdims=True)
    idx[...] = jnp.broadcast_to(ids, (slots, 128))
    cold_load.wait()

    def give(peer, src):
        return pltpu.make_async_remote_copy(
            src_ref=rows_out.at[peer], dst_ref=rows_in.at[src], send_sem=msems.at[2], recv_sem=msems.at[3],
            device_id=device(peer), device_id_type=MESH,
        )

    def serve(first, second):
        group = total // side
        spans = [lax.rem(me_x + dx, side) for dx in (first, second)]
        mine = jnp.concatenate(
            [idx[pl.ds(pl.multiple_of(x * group * 4, group * 4), group * 4), :] for x in spans], axis=0
        )
        sweep(mine, cold, cold_count)
        for c, x in enumerate(spans):
            share = gat[c * group * 4:(c + 1) * group * 4, :].astype(bf)
            rows_out[pl.ds(x * group, group)] = share.reshape(group, 4, share.shape[1])

        def start_give(step, inner):
            for dx in (first, second):
                for core in range(2):
                    peer = peer_at(dx, core, step)

                    @pl.when(peer != me)
                    def _():
                        give(peer, me).start()
            return inner

        lax.fori_loop(0, n, start_give, 0)

    serve(2, 1)
    serve(3, 0)
    rows_in[me] = rows_out[me]
    ask_all.wait_send()
    info_all.wait_recv()
    hot_all.wait_recv()

    def unpack_hot(src, carry):
        pick = unpacker(info_ref[src][1:2], 0, half)
        part[src] = jnp.dot(recv[src, :, 0:half], pick, preferred_element_type=f32).astype(bf)
        return carry

    lax.fori_loop(0, n, unpack_hot, 0, unroll=2)
    row_all.wait_recv()
    flat[...] = rows_in[...].reshape(flat.shape)
    pick = one_hot(packed[half:tokens], float(hot_count), slots)
    found = jnp.dot(pick, flat[...], preferred_element_type=f32).astype(bf)
    emb_packed[half:tokens] = found
    project(1, normalize(found))
    pick = one_hot(rank_t[...], 0.0, tokens)
    emb_ref[...] = jnp.dot(pick, emb_packed[...], preferred_element_type=f32).astype(bf)
    pick = unpacker(info[1:2], 0, tokens)
    opened = jnp.dot(gates[...].reshape(tokens, tokens), pick, preferred_element_type=f32).astype(bf)
    gate_ref[...] = opened.reshape(gate_ref.shape)

    def unpack_cold(src):
        pick = unpacker(info_ref[src][1:2], half, half)
        more = jnp.dot(recv[src, :, half:tokens], pick, preferred_element_type=f32)
        whole = part[src].astype(f32) + more
        v_ref[src] = whole[0:32].astype(bf)
        q_ref[src, 0:32] = (whole[32:64] * scale).astype(bf)
        row = lax.broadcasted_iota(jnp.int32, (16, tokens), 0).astype(f32)
        same = jnp.where(info_ref[src][0:1] == row, 1.0, 0.0)
        q_ref[src, 32:48] = same.astype(bf)
        bias = jnp.where(row < 4.0, (1.0 - same) * (-BIG), 0.0)
        extended = jnp.concatenate([whole[64:96], bias], axis=0).astype(bf)
        k_ref[pl.ds(pl.multiple_of(src * tokens, tokens), tokens), :] = extended.T

    causal = lax.broadcasted_iota(jnp.int32, (half, half), 0) <= lax.broadcasted_iota(jnp.int32, (half, half), 1)

    def attend_own(src):
        q = q_ref[src]
        v = v_ref[src]
        first = pl.multiple_of(src * tokens, tokens)
        early = k_ref[pl.ds(first, half), :]
        late = k_ref[pl.ds(pl.multiple_of(first + half, half), half), :]
        early = silu_half(jnp.dot(early, q, preferred_element_type=f32))
        late = silu_half(jnp.dot(late, q[:, half:], preferred_element_type=f32))
        zero = jnp.zeros((half, half), bf)
        weights[0:half, 0:half] = jnp.where(causal, early[:, 0:half], zero)
        weights[0:half, half:] = early[:, half:]
        weights[half:, half:] = jnp.where(causal, late, zero)
        own_ref[src, :, 0:half] = jnp.dot(v[:, 0:half], weights[0:half, 0:half], preferred_element_type=f32)
        own_ref[src, :, half:] = jnp.dot(v, weights[:, half:], preferred_element_type=f32)

    unpack_cold(me_s)

    def arrive(step, before):
        dz, dy = away(step)
        src = lax.rem(me_z + side - dz, side) * side + lax.rem(me_y + side - dy, side)
        part_copy(1, src, src).wait_recv()
        attend_own(before)
        unpack_cold(src)
        return src

    attend_own(lax.fori_loop(0, n - 1, arrive, me_s))
    row_all.wait_send()
    info_all.wait_send()
    hot_all.wait_send()
    cold_all.wait_send()


def front(token_rows, segment_ids, requests, hot_table, cold_table, weight, n, m):
    tokens = token_rows.shape[1]
    width = hot_table.shape[1]
    total = n * m
    slots = total * requests.shape[1]
    bf = jnp.bfloat16
    f32 = jnp.float32
    vm = pl.BlockSpec(memory_space=pltpu.VMEM)
    hbm = pl.BlockSpec(memory_space=pltpu.HBM)
    operands = (token_rows, segment_ids, requests, hot_table, cold_table, weight)
    return pl.pallas_call(
        functools.partial(front_kernel, n, m),
        out_shape=(
            jax.ShapeDtypeStruct((tokens, width), bf),
            jax.ShapeDtypeStruct((n, 32, tokens), bf),
            jax.ShapeDtypeStruct((n, 48, tokens), bf),
            jax.ShapeDtypeStruct((n * tokens, 48), bf),
            jax.ShapeDtypeStruct((n, 32, tokens), bf),
            jax.ShapeDtypeStruct((n, 2, tokens), f32),
            jax.ShapeDtypeStruct((n, 32, tokens), f32),
        ),
        in_specs=[hbm] * 6,
        out_specs=(vm,) * 7,
        scratch_shapes=[
            pltpu.VMEM((tokens, tokens), bf),
            pltpu.VMEM((n, 96, tokens), bf),
            pltpu.VMEM(token_rows.shape, jnp.int32),
            pltpu.VMEM(segment_ids.shape, jnp.int32),
            pltpu.VMEM(requests.shape, jnp.int32),
            pltpu.VMEM(hot_table.shape, bf),
            pltpu.VMEM(cold_table.shape, bf),
            pltpu.VMEM(weight.shape, bf),
            pltpu.VMEM((n, 96, tokens), bf),
            pltpu.VMEM((n, 96, tokens), bf),
            pltpu.VMEM((n, 32, tokens), bf),
            pltpu.VMEM((tokens, width), bf),
            pltpu.VMEM((2, tokens), f32),
            pltpu.VMEM((total, 1, 128), f32),
            pltpu.VMEM((total, 1, 128), f32),
            pltpu.VMEM((total, 4, width), bf),
            pltpu.VMEM((total, 4, width), bf),
            pltpu.VMEM((slots // 2, width), f32),
            pltpu.VMEM((tokens, 128), f32),
            pltpu.VMEM((tokens, 128), f32),
            pltpu.VMEM((slots, 128), f32),
            pltpu.VMEM((slots, width), bf),
            pltpu.SemaphoreType.DMA((9,)),
            pltpu.SemaphoreType.DMA((n,)),
            pltpu.SemaphoreType.DMA((6,)),
        ],
        compiler_params=pltpu.CompilerParams(collective_id=1, has_side_effects=True, vmem_limit_bytes=46 << 20),
        name="front",
    )(*[pltpu.with_memory_space_constraint(x, pltpu.HBM) for x in operands])


def greet(axis_size):
    me = lax.axis_index("seq")
    barrier = pltpu.get_barrier_semaphore()

    def signal(step, carry):
        peer = lax.rem(me + step, axis_size)
        pl.semaphore_signal(barrier, inc=1, device_id={"seq": peer}, device_id_type=MESH)
        return carry

    lax.fori_loop(1, axis_size, signal, 0)
    pl.semaphore_wait(barrier, axis_size - 1)


def finish_kernel(n, att_ref, gate_ref, emb_ref, wo, up, down, out_ref, back, open_gate, sends, recvs):
    me = lax.axis_index("seq")
    greet(n)

    tokens = emb_ref.shape[0]
    rows = tokens // 2

    def copy_to(part, peer):
        return pltpu.make_async_remote_copy(
            src_ref=att_ref.at[peer, :, pl.ds(part * rows, rows)], dst_ref=back.at[part, me], send_sem=sends,
            recv_sem=recvs.at[part], device_id={"seq": peer}, device_id_type=MESH,
        )

    side = 4
    far = (2, 1, 3, 0)
    for part in range(2):
        for dz in far:
            for dy in far:
                if (dz, dy) != (0, 0):
                    copy_to(part, lax.rem(me // side + dz, side) * side + lax.rem(me + dy, side)).start()
    for part in range(2):
        back[part, me] = att_ref[me, :, part * rows:(part + 1) * rows]

    def open_one(step, carry):
        gate = gate_ref[step].astype(jnp.float32)
        open_gate[step] = gate / (1.0 + jnp.exp(-gate))
        return carry

    lax.fori_loop(0, n, open_one, 0)

    every = pl.ds(0, n - 1)

    def tail(step):
        span = slice(step * rows, (step + 1) * rows)
        pltpu.make_async_remote_copy(
            src_ref=back.at[step, every], dst_ref=back.at[step, every], send_sem=sends, recv_sem=recvs.at[step],
            device_id={"seq": me}, device_id_type=MESH,
        ).wait_recv()
        att = back[step].reshape(n * 32, rows).astype(jnp.float32)
        gate = open_gate[:, :, span].reshape(n * 32, rows)
        scale = lax.rsqrt(jnp.mean(att * att, axis=0, keepdims=True) + epsilon)
        heads = (att * scale * gate).astype(jnp.bfloat16).T
        hidden = emb_ref[span, :].astype(jnp.float32) + jnp.dot(heads, wo[...], preferred_element_type=jnp.float32)
        normed = (hidden * lax.rsqrt(jnp.mean(hidden * hidden, axis=-1, keepdims=True) + epsilon)).astype(jnp.bfloat16)
        wide = jnp.dot(normed, up[...], preferred_element_type=jnp.float32)
        active = (wide / (1.0 + jnp.exp(-wide))).astype(jnp.bfloat16)
        out = hidden + jnp.dot(active, down[...], preferred_element_type=jnp.float32)
        out_ref[span, :] = out.astype(jnp.bfloat16)

    for step in range(2):
        tail(step)
    pltpu.make_async_remote_copy(
        src_ref=att_ref.at[every], dst_ref=att_ref.at[every], send_sem=sends, recv_sem=recvs.at[0],
        device_id={"seq": me}, device_id_type=MESH,
    ).wait_send()


def finish_layer(attended, gate, embedded, wo, up, down, n):
    tokens, width = embedded.shape
    bf = jnp.bfloat16
    vm = pl.BlockSpec(memory_space=pltpu.VMEM)
    return pl.pallas_call(
        functools.partial(finish_kernel, n),
        out_shape=jax.ShapeDtypeStruct((tokens, width), bf),
        in_specs=[vm] * 6,
        out_specs=vm,
        scratch_shapes=[
            pltpu.VMEM((2, n, 32, tokens // 2), bf),
            pltpu.VMEM((n, 32, tokens), jnp.float32),
            pltpu.SemaphoreType.DMA,
            pltpu.SemaphoreType.DMA((2,)),
        ],
        compiler_params=pltpu.CompilerParams(collective_id=2, has_side_effects=True, vmem_limit_bytes=20 << 20),
        name="finish",
    )(attended, gate, embedded, wo, up, down)


def local(token_rows, segment_ids, requests, hot_table, cold_table, input_weight, output_weight, up_weight, down_weight):
    n = lax.axis_size("seq")
    m = lax.axis_size("emb")
    embedded, gate, q, k, v, info, own = front(
        token_rows, segment_ids, jnp.transpose(requests, (0, 2, 1)), hot_table, cold_table, input_weight, n, m
    )
    attended = attention(info, q, k, v, own, 16)
    return finish_layer(attended, gate, embedded, output_weight, up_weight, down_weight, n)[None]


def solution(mesh):
    placed = (
        P("emb", "seq"), P("emb", "seq"), P(("emb", "seq"), None, None), P(), P(("emb", "seq"), None), P(), P(), P(), P(),
    )
    return jax.shard_map(local, mesh=mesh, in_specs=placed, out_specs=P("emb", "seq", None), check_vma=False)
```

```python
import functools

import jax
import jax.numpy as jnp
from jax import lax
from jax.experimental import pallas as pl
from jax.experimental.pallas import tpu as pltpu
from jax.sharding import PartitionSpec as P

epsilon = 1e-06

BIG = float(2 ** 30)


def silu_half(s):
    h = s.astype(jnp.bfloat16)
    return h + h * jnp.tanh(h)


def attn_kernel(U, info_ref, q_ref, k_ref, v_ref, own_ref, out_ref, a_scr, accs):
    blocks, _, W = q_ref.shape
    bf = jnp.bfloat16
    f32 = jnp.float32
    half = W // 2
    segments = info_ref[:, 0:1, :]
    s1, s2, s3 = [jnp.sum((segments < s).astype(f32)).astype(jnp.int32) for s in (1, 2, 3)]
    for i in range(blocks):
        accs[i] = own_ref[i]
    accs[blocks] = jnp.zeros(accs.shape[1:], f32)

    def low(i):
        first = i * W
        start = jnp.where(first >= s3, s3, jnp.where(first >= s2, s2, jnp.where(first >= s1, s1, 0)))
        return jnp.minimum(start // half, 2 * i - 1)

    total = lax.fori_loop(1, blocks, lambda i, c: c + (2 * i - low(i)), 0)

    def after(i, j):
        last = j <= low(i)
        return jnp.where(last, i + 1, i), jnp.where(last, 2 * i + 1, j - 1)

    def weigh(slot, i, j, valid):
        i = jnp.where(valid, i, 0)
        j = jnp.where(valid, j, 0)
        keys = k_ref[pl.ds(pl.multiple_of(j * half, half), half), :]
        a_scr[slot] = silu_half(jnp.dot(keys, q_ref[i], preferred_element_type=f32))

    def gather(slot, i, j, valid):
        i = jnp.where(valid, i, blocks)
        j = jnp.where(valid, j, 0)
        values = v_ref[j // 2, :, pl.ds(pl.multiple_of(lax.rem(j, 2) * half, half), half)]
        accs[i] = accs[i] + jnp.dot(values, a_scr[slot], preferred_element_type=f32)

    def some(n, i, j):
        out = []
        for u in range(U):
            out.append((i, j, n * U + u < total))
            i, j = after(i, j)
        return out, i, j

    one = jnp.int32(1)
    head, i1, j1 = some(0, one, one)
    for u in range(U):
        weigh(u, *head[u])

    def body(n, carry):
        i, j, ni, nj = carry
        now, _, _ = some(n, i, j)
        then, mi, mj = some(n + 1, ni, nj)
        for u in range(U):
            gather(u, *now[u])
            weigh(u, *then[u])
        return ni, nj, mi, mj

    lax.fori_loop(0, (total + U - 1) // U, body, (one, one, i1, j1))
    for i in range(blocks):
        out_ref[i] = accs[i].astype(bf)


def attention(info, q, k, v, own, U):
    blocks, _, W = q.shape
    bf = jnp.bfloat16
    vm = pl.BlockSpec(memory_space=pltpu.VMEM)
    return pl.pallas_call(
        functools.partial(attn_kernel, U),
        out_shape=jax.ShapeDtypeStruct((blocks, 32, W), bf),
        in_specs=[vm] * 5,
        out_specs=vm,
        scratch_shapes=[pltpu.VMEM((U, W // 2, W), bf), pltpu.VMEM((blocks + 1, 32, W), jnp.float32)],
        compiler_params=pltpu.CompilerParams(vmem_limit_bytes=18 << 20),
        name="attn",
    )(info, q, k, v, own)


MESH = pl.DeviceIdType.MESH


def one_hot(ids, base, width):
    lane = lax.broadcasted_iota(jnp.int32, ids.shape, 1).astype(jnp.float32)
    pieces = [
        jnp.where(ids == lane + (base + 128 * c), 1.0, 0.0).astype(jnp.bfloat16) for c in range(width // 128)
    ]
    return jnp.concatenate(pieces, axis=1)


def normalize(values):
    x = values.astype(jnp.float32)
    return (x * lax.rsqrt(jnp.mean(x * x, axis=-1, keepdims=True) + epsilon)).astype(jnp.bfloat16)


def select_exact(pick, ids):
    high = jnp.floor(ids * (1.0 / 64.0))
    low = ids - high * 64.0
    return 64.0 * jnp.dot(pick, high.astype(jnp.bfloat16), preferred_element_type=jnp.float32) + jnp.dot(
        pick, low.astype(jnp.bfloat16), preferred_element_type=jnp.float32
    )


def front_kernel(
    n, m, tok_hbm, seg_hbm, req_hbm, hot_hbm, cold_hbm, w_hbm, emb_ref, gate_ref, q_ref, k_ref, v_ref, info_ref, own_ref,
    weights, part, tok_ref, seg_ref, req_ref, hot, cold, w_ref, send, recv, gates, emb_packed, info, asks, asked,
    rows_out, rows_in, gat, packed, rank_t, idx, flat, msems, crecvs, lsems,
):
    side = 4
    me_s = lax.axis_index("seq")
    me = lax.axis_index("emb") * n + me_s
    me_z, me_y = me_s // side, lax.rem(me_s, side)
    me_x = lax.axis_index("emb") // 2
    total = n * m
    bf = jnp.bfloat16
    f32 = jnp.float32
    hot_count = hot_hbm.shape[0]
    cold_count = cold_hbm.shape[0]
    tokens = tok_hbm.shape[1]
    half = tokens // 2
    slots = idx.shape[0]
    far = (2, 1, 3, 0)
    wide = 4096
    scale = 0.5 / (32.0 ** 0.5)

    barrier = pltpu.get_barrier_semaphore()
    small = [
        pltpu.make_async_copy(a, b, lsems.at[3 + c])
        for c, (a, b) in enumerate(((tok_hbm, tok_ref), (req_hbm, req_ref), (seg_hbm, seg_ref)))
    ]
    for load in small:
        load.start()

    def device(peer):
        return {"emb": peer // n, "seq": lax.rem(peer, n)}

    def away(step):
        t = step // side
        u = lax.rem(step, side)
        dz = lax.rem(2 + 3 * t + 3 * (t // 2) + 2 * (t // 3), side)
        dy = lax.rem(2 + 3 * u + 3 * (u // 2) + 2 * (u // 3), side)
        return dz, dy

    columns = [[lax.rem(me_x + dx, side) * 2 + core for core in range(2)] for dx in range(side)]
    lanes_y = [lax.rem(me_y + dy, side) for dy in range(side)]

    def to_each(act, offsets):
        def plane(t, carry):
            z = lax.rem(me_z + lax.rem(2 + 3 * t + 3 * (t // 2) + 2 * (t // 3), side), side) * side
            for dy in far:
                seq = z + lanes_y[dy]
                for dx in offsets:
                    for emb in columns[dx]:
                        if dx == 0 and dy == 0:

                            @pl.when(emb * n + seq != me)
                            def _():
                                act(emb, seq)
                        else:
                            act(emb, seq)
            return carry

        lax.fori_loop(0, side, plane, 0)

    def signal(emb, seq):
        pl.semaphore_signal(barrier, inc=1, device_id={"emb": emb, "seq": seq}, device_id_type=MESH)

    to_each(signal, far)
    hot_load = pltpu.make_async_copy(hot_hbm, hot, lsems.at[0])
    cold_load = pltpu.make_async_copy(cold_hbm, cold, lsems.at[1])
    w_load = pltpu.make_async_copy(w_hbm, w_ref, lsems.at[2])
    hot_load.start()
    w_load.start()
    cold_load.start()
    for load in small:
        load.wait()
    wanted = req_ref[0].astype(f32)
    wanted = jnp.concatenate([wanted, jnp.zeros((total - wanted.shape[0], total), f32)], axis=0).T
    asks[...] = wanted.reshape(total, 1, total)
    tok = tok_ref[...].astype(f32)
    is_hot = tok < float(hot_count)
    row = lax.broadcasted_iota(jnp.int32, (tokens, tokens), 0)
    earlier = row < lax.broadcasted_iota(jnp.int32, (tokens, tokens), 1)
    marks = jnp.broadcast_to(jnp.where(is_hot, 1.0, 0.0), (8, tokens)).astype(bf)
    before = jnp.dot(marks, jnp.where(earlier, 1.0, 0.0).astype(bf), preferred_element_type=f32)[0:1]
    place = lax.broadcasted_iota(jnp.int32, (1, tokens), 1).astype(f32)
    rank = jnp.where(is_hot, before, half + place - before)
    info[0:1] = seg_ref[...].astype(f32)
    info[1:2] = rank
    rank_t[...] = jnp.broadcast_to(rank, (128, tokens)).T

    def unpacker(ranks, first, count):
        packed_row = lax.broadcasted_iota(jnp.int32, (count, tokens), 0).astype(f32) + float(first)
        return jnp.where(packed_row == ranks, 1.0, 0.0).astype(bf)

    packed[...] = select_exact(unpacker(rank, 0, tokens), jnp.broadcast_to(tok, (128, tokens)).T)
    pl.semaphore_wait(barrier, total - 1)

    def ask(emb, seq):
        pltpu.make_async_remote_copy(
            src_ref=asks.at[emb * n + seq], dst_ref=asked.at[me], send_sem=msems.at[0], recv_sem=msems.at[1],
            device_id={"emb": emb, "seq": seq}, device_id_type=MESH,
        ).start()

    to_each(ask, far)

    def tell(step, carry):
        pltpu.make_async_remote_copy(
            src_ref=info, dst_ref=info_ref.at[me_s], send_sem=msems.at[4], recv_sem=msems.at[5],
            device_id={"seq": lax.rem(me_s + step, n)}, device_id_type=MESH,
        ).start()
        return carry

    lax.fori_loop(1, n, tell, 0)
    asked[me] = asks[me]
    info_ref[me_s] = info[...]

    def sweep(ids, table, count):
        gat[...] = jnp.zeros_like(gat)

        def add(step, inner):
            base = step * wide
            pick = one_hot(ids, base.astype(f32), wide)
            block = table[pl.ds(pl.multiple_of(base, wide), wide), :]
            gat[...] += jnp.dot(pick, block, preferred_element_type=f32)
            return inner

        lax.fori_loop(0, count // wide, add, 0)

    def part_copy(piece, peer, src):
        span = pl.ds(piece * half, half)
        return pltpu.make_async_remote_copy(
            src_ref=send.at[peer, :, span], dst_ref=recv.at[src, :, span], send_sem=msems.at[6 + piece],
            recv_sem=msems.at[8] if piece == 0 else crecvs.at[src],
            device_id={"seq": peer}, device_id_type=MESH,
        )

    def project(piece, x):
        span = slice(piece * half, piece * half + half)
        for dz in far:
            z = lax.rem(me_z + dz, side)
            block = w_ref[:, pl.ds(pl.multiple_of(z * 512, 512), 512)]
            out = jnp.dot(x, block, preferred_element_type=f32).astype(bf).T
            for y in range(side):
                gates[z * side + y, :, span] = out[y * 128:y * 128 + 32]
                send[z * side + y, :, span] = out[y * 128 + 32:y * 128 + 128]
            for dy in far:
                if (dz, dy) != (0, 0):
                    part_copy(piece, z * side + lax.rem(me_y + dy, side), me_s).start()
        recv[me_s, :, span] = send[me_s, :, span]

    hot_load.wait()
    sweep(packed[0:half], hot, hot_count)
    found = gat[...].astype(bf)
    emb_packed[0:half] = found
    w_load.wait()
    project(0, normalize(found))

    def all_of(src, dst, count, a, b, span=None):
        every = pl.ds(0, count)
        src = src.at[every] if span is None else src.at[every, :, span]
        dst = dst.at[every] if span is None else dst.at[every, :, span]
        return pltpu.make_async_remote_copy(
            src_ref=src, dst_ref=dst, send_sem=msems.at[a], recv_sem=msems.at[b],
            device_id=device(me), device_id_type=MESH,
        )

    ask_all = all_of(asks, asked, total - 1, 0, 1)
    row_all = all_of(rows_out, rows_in, total - 1, 2, 3)
    info_all = all_of(info_ref, info_ref, n - 1, 4, 5)
    hot_all = all_of(send, recv, n - 1, 6, 8, pl.ds(0, half))
    cold_all = all_of(send, recv, n - 1, 7, 8, pl.ds(half, half))
    ask_all.wait_recv()
    slot = lax.broadcasted_iota(jnp.int32, (slots, 128), 0)
    lane = lax.broadcasted_iota(jnp.int32, (slots, 128), 1)
    ids = select_exact(jnp.where(slot // 4 == lane, 1.0, 0.0).astype(bf), asked[...].reshape(total, 128))
    ids = jnp.sum(jnp.where(lax.rem(slot, 4) == lane, ids, 0.0), axis=1, keepdims=True)
    idx[...] = jnp.broadcast_to(ids, (slots, 128))
    cold_load.wait()

    def give(emb, seq):
        pltpu.make_async_remote_copy(
            src_ref=rows_out.at[emb * n + seq], dst_ref=rows_in.at[me], send_sem=msems.at[2], recv_sem=msems.at[3],
            device_id={"emb": emb, "seq": seq}, device_id_type=MESH,
        ).start()

    def serve(first, second):
        group = total // side
        spans = [lax.rem(me_x + dx, side) for dx in (first, second)]
        mine = jnp.concatenate(
            [idx[pl.ds(pl.multiple_of(x * group * 4, group * 4), group * 4), :] for x in spans], axis=0
        )
        sweep(mine, cold, cold_count)
        for c, x in enumerate(spans):
            share = gat[c * group * 4:(c + 1) * group * 4, :].astype(bf)
            rows_out[pl.ds(x * group, group)] = share.reshape(group, 4, share.shape[1])

        to_each(give, (first, second))

    serve(2, 1)
    serve(3, 0)
    rows_in[me] = rows_out[me]
    ask_all.wait_send()
    info_all.wait_recv()
    hot_all.wait_recv()

    def unpack_hot(src, carry):
        pick = unpacker(info_ref[src][1:2], 0, half)
        part[src] = jnp.dot(recv[src, :, 0:half], pick, preferred_element_type=f32).astype(bf)
        return carry

    lax.fori_loop(0, n, unpack_hot, 0, unroll=2)
    row_all.wait_recv()
    flat[...] = rows_in[...].reshape(flat.shape)
    pick = one_hot(packed[half:tokens], float(hot_count), slots)
    found = jnp.dot(pick, flat[...], preferred_element_type=f32).astype(bf)
    emb_packed[half:tokens] = found
    project(1, normalize(found))
    pick = one_hot(rank_t[...], 0.0, tokens)
    emb_ref[...] = jnp.dot(pick, emb_packed[...], preferred_element_type=f32).astype(bf)
    pick = unpacker(info[1:2], 0, tokens)
    opened = jnp.dot(gates[...].reshape(tokens, tokens), pick, preferred_element_type=f32).astype(bf)
    gate_ref[...] = opened.reshape(gate_ref.shape)

    def unpack_cold(src):
        pick = unpacker(info_ref[src][1:2], half, half)
        more = jnp.dot(recv[src, :, half:tokens], pick, preferred_element_type=f32)
        whole = part[src].astype(f32) + more
        v_ref[src] = whole[0:32].astype(bf)
        q_ref[src, 0:32] = (whole[32:64] * scale).astype(bf)
        row = lax.broadcasted_iota(jnp.int32, (16, tokens), 0).astype(f32)
        same = jnp.where(info_ref[src][0:1] == row, 1.0, 0.0)
        q_ref[src, 32:48] = same.astype(bf)
        bias = jnp.where(row < 4.0, (1.0 - same) * (-BIG), 0.0)
        extended = jnp.concatenate([whole[64:96], bias], axis=0).astype(bf)
        k_ref[pl.ds(pl.multiple_of(src * tokens, tokens), tokens), :] = extended.T

    causal = lax.broadcasted_iota(jnp.int32, (half, half), 0) <= lax.broadcasted_iota(jnp.int32, (half, half), 1)

    def attend_own(src, slot):
        q = q_ref[src]
        v = v_ref[src]
        first = pl.multiple_of(src * tokens, tokens)
        early = k_ref[pl.ds(first, half), :]
        late = k_ref[pl.ds(pl.multiple_of(first + half, half), half), :]
        early = silu_half(jnp.dot(early, q, preferred_element_type=f32))
        late = silu_half(jnp.dot(late, q[:, half:], preferred_element_type=f32))
        zero = jnp.zeros((half, half), bf)
        weights[slot, 0:half, 0:half] = jnp.where(causal, early[:, 0:half], zero)
        weights[slot, 0:half, half:] = early[:, half:]
        weights[slot, half:, half:] = jnp.where(causal, late, zero)
        own_ref[src, :, 0:half] = jnp.dot(v[:, 0:half], weights[slot, 0:half, 0:half], preferred_element_type=f32)
        own_ref[src, :, half:] = jnp.dot(v, weights[slot, :, half:], preferred_element_type=f32)

    def source(step):
        dz, dy = away(step)
        return lax.rem(me_z + side - dz, side) * side + lax.rem(me_y + side - dy, side)

    def arrive(step, before):
        now = [source(2 * step + 1), source(2 * step + 2)]
        for src in now:
            part_copy(1, src, src).wait_recv()
        for slot in range(2):
            attend_own(before[slot], slot)
        for src in now:
            unpack_cold(src)
        return tuple(now)

    unpack_cold(me_s)
    start = source(0)
    part_copy(1, start, start).wait_recv()
    unpack_cold(start)
    last = lax.fori_loop(0, n // 2 - 1, arrive, (me_s, start))
    for slot in range(2):
        attend_own(last[slot], slot)
    row_all.wait_send()
    info_all.wait_send()
    hot_all.wait_send()
    cold_all.wait_send()


def front(token_rows, segment_ids, requests, hot_table, cold_table, weight, n, m):
    tokens = token_rows.shape[1]
    width = hot_table.shape[1]
    total = n * m
    slots = total * requests.shape[1]
    bf = jnp.bfloat16
    f32 = jnp.float32
    vm = pl.BlockSpec(memory_space=pltpu.VMEM)
    hbm = pl.BlockSpec(memory_space=pltpu.HBM)
    operands = (token_rows, segment_ids, requests, hot_table, cold_table, weight)
    return pl.pallas_call(
        functools.partial(front_kernel, n, m),
        out_shape=(
            jax.ShapeDtypeStruct((tokens, width), bf),
            jax.ShapeDtypeStruct((n, 32, tokens), bf),
            jax.ShapeDtypeStruct((n, 48, tokens), bf),
            jax.ShapeDtypeStruct((n * tokens, 48), bf),
            jax.ShapeDtypeStruct((n, 32, tokens), bf),
            jax.ShapeDtypeStruct((n, 2, tokens), f32),
            jax.ShapeDtypeStruct((n, 32, tokens), f32),
        ),
        in_specs=[hbm] * 6,
        out_specs=(vm,) * 7,
        scratch_shapes=[
            pltpu.VMEM((2, tokens, tokens), bf),
            pltpu.VMEM((n, 96, tokens), bf),
            pltpu.VMEM(token_rows.shape, jnp.int32),
            pltpu.VMEM(segment_ids.shape, jnp.int32),
            pltpu.VMEM(requests.shape, jnp.int32),
            pltpu.VMEM(hot_table.shape, bf),
            pltpu.VMEM(cold_table.shape, bf),
            pltpu.VMEM(weight.shape, bf),
            pltpu.VMEM((n, 96, tokens), bf),
            pltpu.VMEM((n, 96, tokens), bf),
            pltpu.VMEM((n, 32, tokens), bf),
            pltpu.VMEM((tokens, width), bf),
            pltpu.VMEM((2, tokens), f32),
            pltpu.VMEM((total, 1, 128), f32),
            pltpu.VMEM((total, 1, 128), f32),
            pltpu.VMEM((total, 4, width), bf),
            pltpu.VMEM((total, 4, width), bf),
            pltpu.VMEM((slots // 2, width), f32),
            pltpu.VMEM((tokens, 128), f32),
            pltpu.VMEM((tokens, 128), f32),
            pltpu.VMEM((slots, 128), f32),
            pltpu.VMEM((slots, width), bf),
            pltpu.SemaphoreType.DMA((9,)),
            pltpu.SemaphoreType.DMA((n,)),
            pltpu.SemaphoreType.DMA((6,)),
        ],
        compiler_params=pltpu.CompilerParams(collective_id=1, has_side_effects=True, vmem_limit_bytes=46 << 20),
        name="front",
    )(*[pltpu.with_memory_space_constraint(x, pltpu.HBM) for x in operands])


def greet(axis_size):
    me = lax.axis_index("seq")
    barrier = pltpu.get_barrier_semaphore()

    def signal(step, carry):
        peer = lax.rem(me + step, axis_size)
        pl.semaphore_signal(barrier, inc=1, device_id={"seq": peer}, device_id_type=MESH)
        return carry

    lax.fori_loop(1, axis_size, signal, 0)
    pl.semaphore_wait(barrier, axis_size - 1)


def finish_kernel(n, att_ref, gate_ref, emb_ref, wo, up, down, out_ref, back, open_gate, sends, recvs):
    me = lax.axis_index("seq")
    greet(n)

    tokens = emb_ref.shape[0]
    rows = tokens // 2

    def copy_to(part, peer):
        return pltpu.make_async_remote_copy(
            src_ref=att_ref.at[peer, :, pl.ds(part * rows, rows)], dst_ref=back.at[part, me], send_sem=sends,
            recv_sem=recvs.at[part], device_id={"seq": peer}, device_id_type=MESH,
        )

    side = 4
    far = (2, 1, 3, 0)
    for part in range(2):
        for dz in far:
            for dy in far:
                if (dz, dy) != (0, 0):
                    copy_to(part, lax.rem(me // side + dz, side) * side + lax.rem(me + dy, side)).start()
    for part in range(2):
        back[part, me] = att_ref[me, :, part * rows:(part + 1) * rows]

    def open_one(step, carry):
        gate = gate_ref[step].astype(jnp.float32)
        open_gate[step] = gate / (1.0 + jnp.exp(-gate))
        return carry

    lax.fori_loop(0, n, open_one, 0)

    every = pl.ds(0, n - 1)

    def tail(step):
        span = slice(step * rows, (step + 1) * rows)
        pltpu.make_async_remote_copy(
            src_ref=back.at[step, every], dst_ref=back.at[step, every], send_sem=sends, recv_sem=recvs.at[step],
            device_id={"seq": me}, device_id_type=MESH,
        ).wait_recv()
        att = back[step].reshape(n * 32, rows).astype(jnp.float32)
        gate = open_gate[:, :, span].reshape(n * 32, rows)
        scale = lax.rsqrt(jnp.mean(att * att, axis=0, keepdims=True) + epsilon)
        heads = (att * scale * gate).astype(jnp.bfloat16).T
        hidden = emb_ref[span, :].astype(jnp.float32) + jnp.dot(heads, wo[...], preferred_element_type=jnp.float32)
        normed = (hidden * lax.rsqrt(jnp.mean(hidden * hidden, axis=-1, keepdims=True) + epsilon)).astype(jnp.bfloat16)
        wide = jnp.dot(normed, up[...], preferred_element_type=jnp.float32)
        active = (wide / (1.0 + jnp.exp(-wide))).astype(jnp.bfloat16)
        out = hidden + jnp.dot(active, down[...], preferred_element_type=jnp.float32)
        out_ref[span, :] = out.astype(jnp.bfloat16)

    for step in range(2):
        tail(step)
    pltpu.make_async_remote_copy(
        src_ref=att_ref.at[every], dst_ref=att_ref.at[every], send_sem=sends, recv_sem=recvs.at[0],
        device_id={"seq": me}, device_id_type=MESH,
    ).wait_send()


def finish_layer(attended, gate, embedded, wo, up, down, n):
    tokens, width = embedded.shape
    bf = jnp.bfloat16
    vm = pl.BlockSpec(memory_space=pltpu.VMEM)
    return pl.pallas_call(
        functools.partial(finish_kernel, n),
        out_shape=jax.ShapeDtypeStruct((tokens, width), bf),
        in_specs=[vm] * 6,
        out_specs=vm,
        scratch_shapes=[
            pltpu.VMEM((2, n, 32, tokens // 2), bf),
            pltpu.VMEM((n, 32, tokens), jnp.float32),
            pltpu.SemaphoreType.DMA,
            pltpu.SemaphoreType.DMA((2,)),
        ],
        compiler_params=pltpu.CompilerParams(collective_id=2, has_side_effects=True, vmem_limit_bytes=20 << 20),
        name="finish",
    )(attended, gate, embedded, wo, up, down)


def local(token_rows, segment_ids, requests, hot_table, cold_table, input_weight, output_weight, up_weight, down_weight):
    n = lax.axis_size("seq")
    m = lax.axis_size("emb")
    embedded, gate, q, k, v, info, own = front(
        token_rows, segment_ids, jnp.transpose(requests, (0, 2, 1)), hot_table, cold_table, input_weight, n, m
    )
    attended = attention(info, q, k, v, own, 16)
    return finish_layer(attended, gate, embedded, output_weight, up_weight, down_weight, n)[None]


def solution(mesh):
    placed = (
        P("emb", "seq"), P("emb", "seq"), P(("emb", "seq"), None, None), P(), P(("emb", "seq"), None), P(), P(), P(), P(),
    )
    return jax.shard_map(local, mesh=mesh, in_specs=placed, out_specs=P("emb", "seq", None), check_vma=False)
```

```python
import functools

import jax
import jax.numpy as jnp
from jax import lax
from jax.experimental import pallas as pl
from jax.experimental.pallas import tpu as pltpu
from jax.sharding import PartitionSpec as P

epsilon = 1e-06

BIG = float(2 ** 30)


def silu_half(s):
    h = s.astype(jnp.bfloat16)
    return h + h * jnp.tanh(h)


def attn_kernel(U, info_ref, q_ref, k_ref, v_ref, own_ref, out_ref, a_scr, accs):
    blocks, _, W = q_ref.shape
    bf = jnp.bfloat16
    f32 = jnp.float32
    half = W // 2
    segments = info_ref[:, 0:1, :]
    s1, s2, s3 = [jnp.sum((segments < s).astype(f32)).astype(jnp.int32) for s in (1, 2, 3)]
    for i in range(blocks):
        accs[i] = own_ref[i]
    accs[blocks] = jnp.zeros(accs.shape[1:], f32)

    def low(i):
        first = i * W
        start = jnp.where(first >= s3, s3, jnp.where(first >= s2, s2, jnp.where(first >= s1, s1, 0)))
        return jnp.minimum(start // half, 2 * i - 1)

    total = lax.fori_loop(1, blocks, lambda i, c: c + (2 * i - low(i)), 0)

    def after(i, j):
        last = j <= low(i)
        return jnp.where(last, i + 1, i), jnp.where(last, 2 * i + 1, j - 1)

    def weigh(slot, i, j, valid):
        i = jnp.where(valid, i, 0)
        j = jnp.where(valid, j, 0)
        keys = k_ref[pl.ds(pl.multiple_of(j * half, half), half), :]
        a_scr[slot] = silu_half(jnp.dot(keys, q_ref[i], preferred_element_type=f32))

    def gather(slot, i, j, valid):
        i = jnp.where(valid, i, blocks)
        j = jnp.where(valid, j, 0)
        values = v_ref[j // 2, :, pl.ds(pl.multiple_of(lax.rem(j, 2) * half, half), half)]
        accs[i] = accs[i] + jnp.dot(values, a_scr[slot], preferred_element_type=f32)

    def some(n, i, j):
        out = []
        for u in range(U):
            out.append((i, j, n * U + u < total))
            i, j = after(i, j)
        return out, i, j

    one = jnp.int32(1)
    head, i1, j1 = some(0, one, one)
    for u in range(U):
        weigh(u, *head[u])

    def body(n, carry):
        i, j, ni, nj = carry
        now, _, _ = some(n, i, j)
        then, mi, mj = some(n + 1, ni, nj)
        for u in range(U):
            gather(u, *now[u])
            weigh(u, *then[u])
        return ni, nj, mi, mj

    lax.fori_loop(0, (total + U - 1) // U, body, (one, one, i1, j1))
    for i in range(blocks):
        out_ref[i] = accs[i].astype(bf)


def attention(info, q, k, v, own, U):
    blocks, _, W = q.shape
    bf = jnp.bfloat16
    vm = pl.BlockSpec(memory_space=pltpu.VMEM)
    return pl.pallas_call(
        functools.partial(attn_kernel, U),
        out_shape=jax.ShapeDtypeStruct((blocks, 32, W), bf),
        in_specs=[vm] * 5,
        out_specs=vm,
        scratch_shapes=[pltpu.VMEM((U, W // 2, W), bf), pltpu.VMEM((blocks + 1, 32, W), jnp.float32)],
        compiler_params=pltpu.CompilerParams(vmem_limit_bytes=18 << 20),
        name="attn",
    )(info, q, k, v, own)


MESH = pl.DeviceIdType.MESH


def one_hot(ids, base, width):
    lane = lax.broadcasted_iota(jnp.int32, ids.shape, 1).astype(jnp.float32)
    pieces = [
        jnp.where(ids == lane + (base + 128 * c), 1.0, 0.0).astype(jnp.bfloat16) for c in range(width // 128)
    ]
    return jnp.concatenate(pieces, axis=1)


def normalize(values):
    x = values.astype(jnp.float32)
    return (x * lax.rsqrt(jnp.mean(x * x, axis=-1, keepdims=True) + epsilon)).astype(jnp.bfloat16)


def select_exact(pick, ids):
    high = jnp.floor(ids * (1.0 / 64.0))
    low = ids - high * 64.0
    return 64.0 * jnp.dot(pick, high.astype(jnp.bfloat16), preferred_element_type=jnp.float32) + jnp.dot(
        pick, low.astype(jnp.bfloat16), preferred_element_type=jnp.float32
    )


def front_kernel(
    n, m, tok_hbm, seg_hbm, req_hbm, hot_hbm, cold_hbm, w_hbm, emb_ref, gate_ref, q_ref, k_ref, v_ref, info_ref, own_ref,
    weights, part, tok_ref, seg_ref, req_ref, hot, cold, w_ref, send, recv, gates, emb_packed, info, asks, asked,
    rows_out, rows_in, gat, packed, rank_t, idx, flat, msems, crecvs, lsems,
):
    side = 4
    me_s = lax.axis_index("seq")
    me = lax.axis_index("emb") * n + me_s
    me_z, me_y = me_s // side, lax.rem(me_s, side)
    me_x = lax.axis_index("emb") // 2
    total = n * m
    bf = jnp.bfloat16
    f32 = jnp.float32
    hot_count = hot_hbm.shape[0]
    cold_count = cold_hbm.shape[0]
    tokens = tok_hbm.shape[1]
    half = tokens // 2
    slots = idx.shape[0]
    far = (2, 1, 3, 0)
    wide = 4096
    scale = 0.5 / (32.0 ** 0.5)

    barrier = pltpu.get_barrier_semaphore()
    small = [
        pltpu.make_async_copy(a, b, lsems.at[3 + c])
        for c, (a, b) in enumerate(((tok_hbm, tok_ref), (req_hbm, req_ref), (seg_hbm, seg_ref)))
    ]
    for load in small:
        load.start()

    def device(peer):
        return {"emb": peer // n, "seq": lax.rem(peer, n)}

    def away(step):
        t = step // side
        u = lax.rem(step, side)
        dz = lax.rem(2 + 3 * t + 3 * (t // 2) + 2 * (t // 3), side)
        dy = lax.rem(2 + 3 * u + 3 * (u // 2) + 2 * (u // 3), side)
        return dz, dy

    columns = [[lax.rem(me_x + dx, side) * 2 + core for core in range(2)] for dx in range(side)]
    lanes_y = [lax.rem(me_y + dy, side) for dy in range(side)]

    def to_each(act, offsets):
        def plane(t, carry):
            z = lax.rem(me_z + lax.rem(2 + 3 * t + 3 * (t // 2) + 2 * (t // 3), side), side) * side
            for dy in far:
                seq = z + lanes_y[dy]
                for dx in offsets:
                    for emb in columns[dx]:
                        if dx == 0 and dy == 0:

                            @pl.when(emb * n + seq != me)
                            def _():
                                act(emb, seq)
                        else:
                            act(emb, seq)
            return carry

        lax.fori_loop(0, side, plane, 0)

    def signal(emb, seq):
        pl.semaphore_signal(barrier, inc=1, device_id={"emb": emb, "seq": seq}, device_id_type=MESH)

    to_each(signal, far)
    hot_load = pltpu.make_async_copy(hot_hbm, hot, lsems.at[0])
    cold_load = pltpu.make_async_copy(cold_hbm, cold, lsems.at[1])
    w_load = pltpu.make_async_copy(w_hbm, w_ref, lsems.at[2])
    hot_load.start()
    w_load.start()
    cold_load.start()
    for load in small:
        load.wait()
    wanted = req_ref[0].astype(f32)
    wanted = jnp.concatenate([wanted, jnp.zeros((total - wanted.shape[0], total), f32)], axis=0).T
    asks[...] = wanted.reshape(total, 1, total)
    tok = tok_ref[...].astype(f32)
    is_hot = tok < float(hot_count)
    row = lax.broadcasted_iota(jnp.int32, (tokens, tokens), 0)
    earlier = row < lax.broadcasted_iota(jnp.int32, (tokens, tokens), 1)
    marks = jnp.broadcast_to(jnp.where(is_hot, 1.0, 0.0), (8, tokens)).astype(bf)
    before = jnp.dot(marks, jnp.where(earlier, 1.0, 0.0).astype(bf), preferred_element_type=f32)[0:1]
    place = lax.broadcasted_iota(jnp.int32, (1, tokens), 1).astype(f32)
    rank = jnp.where(is_hot, before, half + place - before)
    info[0:1] = seg_ref[...].astype(f32)
    info[1:2] = rank
    rank_t[...] = jnp.broadcast_to(rank, (128, tokens)).T

    def unpacker(ranks, first, count):
        packed_row = lax.broadcasted_iota(jnp.int32, (count, tokens), 0).astype(f32) + float(first)
        return jnp.where(packed_row == ranks, 1.0, 0.0).astype(bf)

    packed[...] = select_exact(unpacker(rank, 0, tokens), jnp.broadcast_to(tok, (128, tokens)).T)
    pl.semaphore_wait(barrier, total - 1)

    def ask(emb, seq):
        pltpu.make_async_remote_copy(
            src_ref=asks.at[emb * n + seq], dst_ref=asked.at[me], send_sem=msems.at[0], recv_sem=msems.at[1],
            device_id={"emb": emb, "seq": seq}, device_id_type=MESH,
        ).start()

    to_each(ask, far)

    def tell(step, carry):
        pltpu.make_async_remote_copy(
            src_ref=info, dst_ref=info_ref.at[me_s], send_sem=msems.at[4], recv_sem=msems.at[5],
            device_id={"seq": lax.rem(me_s + step, n)}, device_id_type=MESH,
        ).start()
        return carry

    lax.fori_loop(1, n, tell, 0)
    asked[me] = asks[me]
    info_ref[me_s] = info[...]

    def sweep(ids, table, count):
        gat[...] = jnp.zeros_like(gat)

        def add(step, inner):
            base = step * wide
            pick = one_hot(ids, base.astype(f32), wide)
            block = table[pl.ds(pl.multiple_of(base, wide), wide), :]
            gat[...] += jnp.dot(pick, block, preferred_element_type=f32)
            return inner

        lax.fori_loop(0, count // wide, add, 0)

    def part_copy(piece, peer, src):
        span = pl.ds(piece * half, half)
        return pltpu.make_async_remote_copy(
            src_ref=send.at[peer, :, span], dst_ref=recv.at[src, :, span], send_sem=msems.at[6 + piece],
            recv_sem=msems.at[8] if piece == 0 else crecvs.at[src],
            device_id={"seq": peer}, device_id_type=MESH,
        )

    def project(piece, x):
        span = slice(piece * half, piece * half + half)
        for dz in far:
            z = lax.rem(me_z + dz, side)
            block = w_ref[:, pl.ds(pl.multiple_of(z * 512, 512), 512)]
            out = jnp.dot(x, block, preferred_element_type=f32).astype(bf).T
            for y in range(side):
                gates[z * side + y, :, span] = out[y * 128:y * 128 + 32]
                send[z * side + y, :, span] = out[y * 128 + 32:y * 128 + 128]
            for dy in far:
                if (dz, dy) != (0, 0):
                    part_copy(piece, z * side + lax.rem(me_y + dy, side), me_s).start()
        recv[me_s, :, span] = send[me_s, :, span]

    hot_load.wait()
    sweep(packed[0:half], hot, hot_count)
    found = gat[...].astype(bf)
    emb_packed[0:half] = found
    w_load.wait()
    project(0, normalize(found))

    def all_of(src, dst, count, a, b, span=None):
        every = pl.ds(0, count)
        src = src.at[every] if span is None else src.at[every, :, span]
        dst = dst.at[every] if span is None else dst.at[every, :, span]
        return pltpu.make_async_remote_copy(
            src_ref=src, dst_ref=dst, send_sem=msems.at[a], recv_sem=msems.at[b],
            device_id=device(me), device_id_type=MESH,
        )

    ask_all = all_of(asks, asked, total - 1, 0, 1)
    row_all = all_of(rows_out, rows_in, total - 1, 2, 3)
    info_all = all_of(info_ref, info_ref, n - 1, 4, 5)
    hot_all = all_of(send, recv, n - 1, 6, 8, pl.ds(0, half))
    cold_all = all_of(send, recv, n - 1, 7, 8, pl.ds(half, half))
    ask_all.wait_recv()
    slot = lax.broadcasted_iota(jnp.int32, (slots, 128), 0)
    lane = lax.broadcasted_iota(jnp.int32, (slots, 128), 1)
    ids = select_exact(jnp.where(slot // 4 == lane, 1.0, 0.0).astype(bf), asked[...].reshape(total, 128))
    ids = jnp.sum(jnp.where(lax.rem(slot, 4) == lane, ids, 0.0), axis=1, keepdims=True)
    idx[...] = jnp.broadcast_to(ids, (slots, 128))
    cold_load.wait()

    def give(emb, seq):
        pltpu.make_async_remote_copy(
            src_ref=rows_out.at[emb * n + seq], dst_ref=rows_in.at[me], send_sem=msems.at[2], recv_sem=msems.at[3],
            device_id={"emb": emb, "seq": seq}, device_id_type=MESH,
        ).start()

    def serve(first, second):
        group = total // side
        spans = [lax.rem(me_x + dx, side) for dx in (first, second)]
        mine = jnp.concatenate(
            [idx[pl.ds(pl.multiple_of(x * group * 4, group * 4), group * 4), :] for x in spans], axis=0
        )
        sweep(mine, cold, cold_count)
        for c, x in enumerate(spans):
            share = gat[c * group * 4:(c + 1) * group * 4, :].astype(bf)
            rows_out[pl.ds(x * group, group)] = share.reshape(group, 4, share.shape[1])

        to_each(give, (first, second))

    serve(2, 1)
    serve(3, 0)
    rows_in[me] = rows_out[me]
    ask_all.wait_send()
    info_all.wait_recv()
    hot_all.wait_recv()

    def unpack_hot(src, carry):
        pick = unpacker(info_ref[src][1:2], 0, half)
        part[src] = jnp.dot(recv[src, :, 0:half], pick, preferred_element_type=f32).astype(bf)
        return carry

    lax.fori_loop(0, n, unpack_hot, 0, unroll=2)
    row_all.wait_recv()
    flat[...] = rows_in[...].reshape(flat.shape)
    pick = one_hot(packed[half:tokens], float(hot_count), slots)
    found = jnp.dot(pick, flat[...], preferred_element_type=f32).astype(bf)
    emb_packed[half:tokens] = found
    project(1, normalize(found))
    pick = one_hot(rank_t[...], 0.0, tokens)
    emb_ref[...] = jnp.dot(pick, emb_packed[...], preferred_element_type=f32).astype(bf)
    pick = unpacker(info[1:2], 0, tokens)
    opened = jnp.dot(gates[...].reshape(tokens, tokens), pick, preferred_element_type=f32).astype(bf)
    gate_ref[...] = opened.reshape(gate_ref.shape)

    def unpack_cold(src):
        pick = unpacker(info_ref[src][1:2], half, half)
        more = jnp.dot(recv[src, :, half:tokens], pick, preferred_element_type=f32)
        whole = part[src].astype(f32) + more
        v_ref[src] = whole[0:32].astype(bf)
        q_ref[src, 0:32] = (whole[32:64] * scale).astype(bf)
        row = lax.broadcasted_iota(jnp.int32, (16, tokens), 0).astype(f32)
        same = jnp.where(info_ref[src][0:1] == row, 1.0, 0.0)
        q_ref[src, 32:48] = same.astype(bf)
        bias = jnp.where(row < 4.0, (1.0 - same) * (-BIG), 0.0)
        extended = jnp.concatenate([whole[64:96], bias], axis=0).astype(bf)
        k_ref[pl.ds(pl.multiple_of(src * tokens, tokens), tokens), :] = extended.T

    causal = lax.broadcasted_iota(jnp.int32, (half, half), 0) <= lax.broadcasted_iota(jnp.int32, (half, half), 1)

    def attend_own(src, slot):
        q = q_ref[src]
        v = v_ref[src]
        first = pl.multiple_of(src * tokens, tokens)
        early = k_ref[pl.ds(first, half), :]
        late = k_ref[pl.ds(pl.multiple_of(first + half, half), half), :]
        early = silu_half(jnp.dot(early, q, preferred_element_type=f32))
        late = silu_half(jnp.dot(late, q[:, half:], preferred_element_type=f32))
        zero = jnp.zeros((half, half), bf)
        weights[slot, 0:half, 0:half] = jnp.where(causal, early[:, 0:half], zero)
        weights[slot, 0:half, half:] = early[:, half:]
        weights[slot, half:, half:] = jnp.where(causal, late, zero)
        own_ref[src, :, 0:half] = jnp.dot(v[:, 0:half], weights[slot, 0:half, 0:half], preferred_element_type=f32)
        own_ref[src, :, half:] = jnp.dot(v, weights[slot, :, half:], preferred_element_type=f32)

    def source(step):
        dz, dy = away(step)
        return lax.rem(me_z + side - dz, side) * side + lax.rem(me_y + side - dy, side)

    def arrive(step, before):
        now = [source(2 * step + 1), source(2 * step + 2)]
        for src in now:
            part_copy(1, src, src).wait_recv()
        for slot in range(2):
            attend_own(before[slot], slot)
        for src in now:
            unpack_cold(src)
        return tuple(now)

    unpack_cold(me_s)
    start = source(0)
    part_copy(1, start, start).wait_recv()
    unpack_cold(start)
    last = lax.fori_loop(0, n // 2 - 1, arrive, (me_s, start))
    for slot in range(2):
        attend_own(last[slot], slot)
    row_all.wait_send()
    info_all.wait_send()
    hot_all.wait_send()
    cold_all.wait_send()


def front(token_rows, segment_ids, requests, hot_table, cold_table, weight, n, m):
    tokens = token_rows.shape[1]
    width = hot_table.shape[1]
    total = n * m
    slots = total * requests.shape[1]
    bf = jnp.bfloat16
    f32 = jnp.float32
    vm = pl.BlockSpec(memory_space=pltpu.VMEM)
    hbm = pl.BlockSpec(memory_space=pltpu.HBM)
    operands = (token_rows, segment_ids, requests, hot_table, cold_table, weight)
    return pl.pallas_call(
        functools.partial(front_kernel, n, m),
        out_shape=(
            jax.ShapeDtypeStruct((tokens, width), bf),
            jax.ShapeDtypeStruct((n, 32, tokens), bf),
            jax.ShapeDtypeStruct((n, 48, tokens), bf),
            jax.ShapeDtypeStruct((n * tokens, 48), bf),
            jax.ShapeDtypeStruct((n, 32, tokens), bf),
            jax.ShapeDtypeStruct((n, 2, tokens), f32),
            jax.ShapeDtypeStruct((n, 32, tokens), f32),
        ),
        in_specs=[hbm] * 6,
        out_specs=(vm,) * 7,
        scratch_shapes=[
            pltpu.VMEM((2, tokens, tokens), bf),
            pltpu.VMEM((n, 96, tokens), bf),
            pltpu.VMEM(token_rows.shape, jnp.int32),
            pltpu.VMEM(segment_ids.shape, jnp.int32),
            pltpu.VMEM(requests.shape, jnp.int32),
            pltpu.VMEM(hot_table.shape, bf),
            pltpu.VMEM(cold_table.shape, bf),
            pltpu.VMEM(weight.shape, bf),
            pltpu.VMEM((n, 96, tokens), bf),
            pltpu.VMEM((n, 96, tokens), bf),
            pltpu.VMEM((n, 32, tokens), bf),
            pltpu.VMEM((tokens, width), bf),
            pltpu.VMEM((2, tokens), f32),
            pltpu.VMEM((total, 1, 128), f32),
            pltpu.VMEM((total, 1, 128), f32),
            pltpu.VMEM((total, 4, width), bf),
            pltpu.VMEM((total, 4, width), bf),
            pltpu.VMEM((slots // 2, width), f32),
            pltpu.VMEM((tokens, 128), f32),
            pltpu.VMEM((tokens, 128), f32),
            pltpu.VMEM((slots, 128), f32),
            pltpu.VMEM((slots, width), bf),
            pltpu.SemaphoreType.DMA((9,)),
            pltpu.SemaphoreType.DMA((n,)),
            pltpu.SemaphoreType.DMA((6,)),
        ],
        compiler_params=pltpu.CompilerParams(collective_id=1, has_side_effects=True, vmem_limit_bytes=46 << 20),
        name="front",
    )(*[pltpu.with_memory_space_constraint(x, pltpu.HBM) for x in operands])


def greet(axis_size):
    me = lax.axis_index("seq")
    barrier = pltpu.get_barrier_semaphore()

    def signal(step, carry):
        peer = lax.rem(me + step, axis_size)
        pl.semaphore_signal(barrier, inc=1, device_id={"seq": peer}, device_id_type=MESH)
        return carry

    lax.fori_loop(1, axis_size, signal, 0)
    pl.semaphore_wait(barrier, axis_size - 1)


def finish_kernel(n, att_ref, gate_ref, emb_ref, wo, up, down, out_ref, back, open_gate, sends, recvs):
    me = lax.axis_index("seq")
    greet(n)

    tokens = emb_ref.shape[0]
    rows = tokens // 4

    def copy_to(part, peer):
        return pltpu.make_async_remote_copy(
            src_ref=att_ref.at[peer, :, pl.ds(part * rows, rows)], dst_ref=back.at[part, me], send_sem=sends,
            recv_sem=recvs.at[part], device_id={"seq": peer}, device_id_type=MESH,
        )

    side = 4
    far = (2, 1, 3, 0)
    for part in range(4):
        for dz in far:
            for dy in far:
                if (dz, dy) != (0, 0):
                    copy_to(part, lax.rem(me // side + dz, side) * side + lax.rem(me + dy, side)).start()
    for part in range(4):
        back[part, me] = att_ref[me, :, part * rows:(part + 1) * rows]

    def open_one(step, carry):
        gate = gate_ref[step].astype(jnp.float32)
        open_gate[step] = gate / (1.0 + jnp.exp(-gate))
        return carry

    lax.fori_loop(0, n, open_one, 0)

    every = pl.ds(0, n - 1)

    def tail(step):
        span = slice(step * rows, (step + 1) * rows)
        pltpu.make_async_remote_copy(
            src_ref=back.at[step, every], dst_ref=back.at[step, every], send_sem=sends, recv_sem=recvs.at[step],
            device_id={"seq": me}, device_id_type=MESH,
        ).wait_recv()
        att = back[step].reshape(n * 32, rows).astype(jnp.float32)
        gate = open_gate[:, :, span].reshape(n * 32, rows)
        scale = lax.rsqrt(jnp.mean(att * att, axis=0, keepdims=True) + epsilon)
        heads = (att * scale * gate).astype(jnp.bfloat16).T
        hidden = emb_ref[span, :].astype(jnp.float32) + jnp.dot(heads, wo[...], preferred_element_type=jnp.float32)
        normed = (hidden * lax.rsqrt(jnp.mean(hidden * hidden, axis=-1, keepdims=True) + epsilon)).astype(jnp.bfloat16)
        wide = jnp.dot(normed, up[...], preferred_element_type=jnp.float32)
        active = (wide / (1.0 + jnp.exp(-wide))).astype(jnp.bfloat16)
        out = hidden + jnp.dot(active, down[...], preferred_element_type=jnp.float32)
        out_ref[span, :] = out.astype(jnp.bfloat16)

    for step in range(4):
        tail(step)
    pltpu.make_async_remote_copy(
        src_ref=att_ref.at[every], dst_ref=att_ref.at[every], send_sem=sends, recv_sem=recvs.at[0],
        device_id={"seq": me}, device_id_type=MESH,
    ).wait_send()


def finish_layer(attended, gate, embedded, wo, up, down, n):
    tokens, width = embedded.shape
    bf = jnp.bfloat16
    vm = pl.BlockSpec(memory_space=pltpu.VMEM)
    return pl.pallas_call(
        functools.partial(finish_kernel, n),
        out_shape=jax.ShapeDtypeStruct((tokens, width), bf),
        in_specs=[vm] * 6,
        out_specs=vm,
        scratch_shapes=[
            pltpu.VMEM((4, n, 32, tokens // 4), bf),
            pltpu.VMEM((n, 32, tokens), jnp.float32),
            pltpu.SemaphoreType.DMA,
            pltpu.SemaphoreType.DMA((4,)),
        ],
        compiler_params=pltpu.CompilerParams(collective_id=2, has_side_effects=True, vmem_limit_bytes=20 << 20),
        name="finish",
    )(attended, gate, embedded, wo, up, down)


def local(token_rows, segment_ids, requests, hot_table, cold_table, input_weight, output_weight, up_weight, down_weight):
    n = lax.axis_size("seq")
    m = lax.axis_size("emb")
    embedded, gate, q, k, v, info, own = front(
        token_rows, segment_ids, jnp.transpose(requests, (0, 2, 1)), hot_table, cold_table, input_weight, n, m
    )
    attended = attention(info, q, k, v, own, 16)
    return finish_layer(attended, gate, embedded, output_weight, up_weight, down_weight, n)[None]


def solution(mesh):
    placed = (
        P("emb", "seq"), P("emb", "seq"), P(("emb", "seq"), None, None), P(), P(("emb", "seq"), None), P(), P(), P(), P(),
    )
    return jax.shard_map(local, mesh=mesh, in_specs=placed, out_specs=P("emb", "seq", None), check_vma=False)
```
